8 devices in a mesh: dp: 1 (over z), tp: 2 (over y), ep: 4 (over x, core).
Axes of the slice: x: 2, y: 2, z: 1, core: 2. Of those that a mesh axis runs over, the one named last changes fastest.
Arguments:
- tokens: bfloat16 [1024, 2048], P(('dp', 'ep'))
- logits: float32 [1024, 8], P(('dp', 'ep'))
- w_in: bfloat16 [8, 2048, 5632], P('ep', None, 'tp')
- w_out: bfloat16 [8, 5632, 2048], P('ep', 'tp')
Outputs:
- output: bfloat16 [1024, 2048], P(('dp', 'ep'))
All inputs are finite; a program needn't handle non-finite values.
Results may differ from the reference program's by a relative error of at most 0.001.
Values are sent between devices in bfloat16 or wider.
A program may use at most 1 GiB of HBM per device.

```python
import math
import jax
import jax.numpy as jnp
from jax import lax

TOKENS = 1024
BLOCK_TOKENS = 256
NUM_BLOCKS = 4
MODEL_DIM = 2048
HIDDEN_DIM = 5632
EXPERTS = 8
CAPACITY = 256
CAND_MAX = 128


def route_logits(route_key):
    key_pairs, key_order, key_local, key_code = jax.random.split(route_key, 4)
    pair_count = NUM_BLOCKS // 2
    first_share = jnp.concatenate(
        [jnp.full((EXPERTS, 1), CAND_MAX, jnp.int32),
         jax.random.randint(key_pairs, (EXPERTS, pair_count - 1), 0, CAND_MAX + 1)], axis=1)
    share_pairs = jnp.stack([first_share, CAND_MAX - first_share], axis=2).reshape(EXPERTS, NUM_BLOCKS)
    block_order = jax.vmap(lambda sub_key: jax.random.permutation(sub_key, NUM_BLOCKS))(
        jax.random.split(key_order, EXPERTS))
    block_count = jnp.take_along_axis(share_pairs, block_order, axis=1)
    local_rank = jax.vmap(lambda sub_key: jax.random.permutation(sub_key, BLOCK_TOKENS))(
        jax.random.split(key_local, EXPERTS * NUM_BLOCKS)).reshape(EXPERTS, NUM_BLOCKS, BLOCK_TOKENS)
    chosen = (local_rank < block_count[:, :, None]).reshape(EXPERTS, TOKENS)
    rank_code = jax.vmap(lambda sub_key: jax.random.permutation(sub_key, TOKENS))(
        jax.random.split(key_code, EXPERTS))
    step_size = 2.0 / (2 ** math.ceil(math.log2(TOKENS)))
    band_base = jnp.where(chosen, 2.0, -2.0)
    logits = band_base + rank_code.astype(jnp.float32) * step_size
    return logits.T.astype(jnp.float32)


def setup_inputs(seed: int = 0, part: int = 0) -> dict:
    part_key = jax.random.fold_in(jax.random.key(seed), part)
    key_tokens, key_route = jax.random.split(part_key)
    key_in, key_out = jax.random.split(jax.random.key(seed + 1))
    tokens = jax.random.normal(key_tokens, (TOKENS, MODEL_DIM), jnp.float32).astype(jnp.bfloat16)
    logits = route_logits(key_route)
    w_in = (jax.random.normal(key_in, (EXPERTS, MODEL_DIM, HIDDEN_DIM), jnp.float32)
            * MODEL_DIM ** -0.5).astype(jnp.bfloat16)
    w_out = (jax.random.normal(key_out, (EXPERTS, HIDDEN_DIM, MODEL_DIM), jnp.float32)
             * (2.0 * HIDDEN_DIM ** -0.5)).astype(jnp.bfloat16)
    return {"tokens": tokens, "logits": logits, "w_in": w_in, "w_out": w_out}


def reference(tokens, logits, w_in, w_out):
    gate_probs = jax.nn.softmax(logits, axis=-1)
    _, top_rows = lax.top_k(logits.T, CAPACITY)
    gate_pick = jnp.take_along_axis(gate_probs.T, top_rows, axis=1)

    def expert_step(acc_sum, expert_item):
        pick_rows, gate_w, w_first, w_second = expert_item
        picked = tokens[pick_rows]
        hidden = jax.nn.gelu(jnp.dot(picked, w_first, preferred_element_type=jnp.float32),
                             approximate=True).astype(jnp.bfloat16)
        expert_out = jnp.dot(hidden, w_second, preferred_element_type=jnp.float32).astype(jnp.bfloat16)
        acc_sum = acc_sum.at[pick_rows].add(gate_w[:, None] * expert_out.astype(jnp.float32))
        return acc_sum, None

    mix_sum, _ = lax.scan(expert_step, jnp.zeros((TOKENS, MODEL_DIM), jnp.float32),
                          (top_rows, gate_pick, w_in, w_out))
    return (tokens.astype(jnp.float32) + mix_sum).astype(jnp.bfloat16)
```

```python
import functools

import jax
import jax.numpy as jnp
from jax import lax
from jax.experimental import pallas as pl
from jax.experimental.pallas import tpu as pltpu
from jax.sharding import PartitionSpec as P

MESH = pl.DeviceIdType.MESH
F32 = jnp.float32
BF16 = jnp.bfloat16

BLK = 256
EXPERTS = 8
OWN = 2
CAP = 256
DIM = 2048
HID = 2816
EP = 4
TOK = BLK * EP
HALF = DIM // 2
NK = 4
KC = DIM // NK
NJ = 8
NC = HALF // NJ
NB = 3
TILE = 256


def gelu(v):
    return 0.5 * v * (1.0 + jnp.tanh(v * (0.7978845608028654 + 0.035677408136300125 * (v * v))))


def column(row):
    return jnp.transpose(jnp.broadcast_to(row, (128, 128)))


def kernel(tok, lt, w_in, w_out, out,
           xall, ltall, onehot, xg, win, acc, hid, wout, snd, rcv, zall, back, gate, res,
           loc_sem, win_sem, wout_sem, out_sem,
           lt_s, lt_r, a_s, a_r, b_s, b_r, c_s, c_r, d_s, d_r, e_s, e_r,
           s_s, s_r, zc_s, zc_r, zx_s, zx_r, zf_s, zf_r, res_s, res_r):
    ep = lax.axis_index("ep")
    tp = lax.axis_index("tp")
    near = ep + 1 - 2 * lax.rem(ep, 2)
    far = lax.rem(ep + 2, 4)
    diag = 3 - ep
    peer = 1 - tp
    to_near, to_far, to_diag = {"ep": near, "tp": tp}, {"ep": far, "tp": tp}, {"ep": diag, "tp": tp}
    to_peer = {"ep": ep, "tp": peer}

    def rows(block, half=None):
        if half is None:
            return pl.ds(pl.multiple_of(block * BLK, BLK), BLK)
        return pl.ds(pl.multiple_of(block * BLK + half * (BLK // 2), BLK // 2), BLK // 2)

    def load_tok(k):
        return pltpu.make_async_copy(tok.at[:, pl.ds(k * KC, KC)], xall.at[k, rows(ep)], loc_sem.at[k])

    def load_win(e, k):
        part = pl.ds(k * KC, KC)
        return pltpu.make_async_copy(w_in.at[e, part], win.at[e, part], win_sem.at[e * NK + k])

    def load_wout(j, e, side):
        slot = lax.rem(j, NB)
        half = peer if side == 0 else tp
        cols = pl.ds(pl.multiple_of(half * HALF + j * NC, NC), NC)
        return pltpu.make_async_copy(w_out.at[e, :, cols], wout.at[slot, e, :, pl.ds(side * NC, NC)],
                                     wout_sem.at[slot, 2 * e + side])

    def remote(src, dst, send, recv, where):
        return pltpu.make_async_remote_copy(src_ref=src, dst_ref=dst, send_sem=send, recv_sem=recv,
                                            device_id=where, device_id_type=MESH)

    def moved(ref, k, r, send, recv, where):
        piece = ref.at[k, r]
        return remote(piece, piece, send.at[k], recv.at[k], where)

    def copy_lt(i, where, slot):
        return remote(lt, ltall.at[slot], lt_s.at[i], lt_r.at[i], where)

    def copy_a(k, block):
        return moved(xall, k, rows(block), a_s, a_r, to_near)

    def copy_b(k, block):
        return moved(xall, k, rows(block, tp), b_s, b_r, to_far)

    def copy_c(k, block):
        return moved(xall, k, rows(block, tp), c_s, c_r, to_near)

    def copy_d(k, half):
        return moved(xall, k, rows(far, half), d_s, d_r, to_peer)

    def copy_e(k, block):
        return moved(xall, k, rows(block, peer), e_s, e_r, to_near)

    def copy_s(j):
        return remote(snd.at[j], rcv.at[j], s_s.at[j], s_r.at[j], to_peer)

    def zrows(owner):
        return pl.ds(pl.multiple_of(owner * (OWN * CAP), OWN * CAP), OWN * CAP)

    def copy_zc(j, owner):
        return moved(zall, j, zrows(owner), zc_s, zc_r, to_near)

    def copy_zx(j, owner):
        return moved(zall, j, zrows(owner), zx_s, zx_r, to_far)

    def copy_zf(j, owner):
        return moved(zall, j, zrows(owner), zf_s, zf_r, to_near)

    def out_cols(half, j):
        return out.at[:, pl.ds(pl.multiple_of(half * HALF + j * NC, NC), NC)]

    def copy_res(j, half):
        return remote(res.at[j], out_cols(half, j), res_s.at[j], res_r.at[j], to_peer)

    def store_res(j):
        return pltpu.make_async_copy(res.at[j], out_cols(tp, j), out_sem.at[j])

    for k in range(NK):
        load_tok(k).start()
    for k in range(NK):
        for e in range(OWN):
            load_win(e, k).start()
    for j in range(NB):
        for e in range(OWN):
            for side in range(2):
                load_wout(j, e, side).start()

    barrier = pltpu.get_barrier_semaphore()
    for where in (to_near, to_far, to_diag, to_peer):
        pl.semaphore_signal(barrier, inc=1, device_id=where, device_id_type=MESH)
    pl.semaphore_wait(barrier, 4)

    for i, where in enumerate((to_near, to_far, to_diag)):
        copy_lt(i, where, ep).start()
    for k in range(NK):
        load_tok(k).wait()
        copy_b(k, ep).start()
        copy_a(k, ep).start()

    ltall[ep] = lt[...]
    for i, (where, slot) in enumerate(((to_near, near), (to_far, far), (to_diag, diag))):
        copy_lt(i, where, slot).wait_recv()

    def pick(i, _):
        expert = ep * OWN + i
        line = jnp.concatenate([ltall[b, pl.ds(expert, 1), :] for b in range(EP)], axis=1)
        rank = jnp.zeros((1, TOK), F32)
        for s in range(TOK // 128):
            col = column(line[:, s * 128:(s + 1) * 128])
            wide = jnp.concatenate([col] * (TOK // 128), axis=1)
            rank = rank + jnp.sum(jnp.where(wide > line, 1.0, 0.0), axis=0, keepdims=True)
        slots = lax.broadcasted_iota(jnp.int32, (CAP, TOK), 0).astype(F32)
        onehot[i] = jnp.where(slots == rank, 1.0, 0.0).astype(BF16)
        return 0

    lax.fori_loop(0, OWN, pick, 0)

    def first(k):
        def body(e, _):
            load_win(e, k).wait()
            xg[...] = jnp.dot(onehot[e], xall[k], preferred_element_type=F32).astype(BF16)
            for n in range(HID // TILE):
                cols = slice(n * TILE, (n + 1) * TILE)
                r = jnp.dot(xg[...], win[e, k * KC:(k + 1) * KC, cols], preferred_element_type=F32)
                if k > 0:
                    r = r + acc[e, :, cols]
                if k < NK - 1:
                    acc[e, :, cols] = r
                else:
                    hid[e, :, cols] = gelu(r).astype(BF16)
            return 0
        lax.fori_loop(0, OWN, body, 0)

    def arrive(k):
        copy_a(k, near).wait_recv()
        copy_c(k, diag).wait_recv()
        copy_e(k, diag).wait_recv()

    for k in range(NK + 2):
        if k < NK:
            copy_b(k, far).wait_recv()
            copy_c(k, far).start()
            copy_d(k, tp).start()
        if 0 <= k - 1 < NK:
            copy_d(k - 1, peer).wait_recv()
            copy_e(k - 1, far).start()
        if 0 <= k - 2 < NK:
            arrive(k - 2)
            first(k - 2)

    def second(j, _):
        slot = lax.rem(j, NB)

        def body(e, _):
            for side in range(2):
                load_wout(j, e, side).wait()
            r = jnp.dot(hid[e], wout[slot, e], preferred_element_type=F32)
            place = pl.ds(pl.multiple_of(e * CAP, CAP), CAP)
            snd[j, place, :] = r[:, :NC]
            acc[e, :, pl.ds(pl.multiple_of(j * NC, NC), NC)] = r[:, NC:]
            return 0
        lax.fori_loop(0, OWN, body, 0)
        copy_s(j).start()

        @pl.when(j + NB < NJ)
        def _():
            for e in range(OWN):
                for side in range(2):
                    load_wout(j + NB, e, side).start()
        return 0

    lax.fori_loop(0, NJ, second, 0)

    scores = lt[...]
    top = jnp.max(scores, axis=0, keepdims=True)
    grown = jnp.exp(scores - top)
    probs = grown / jnp.sum(grown, axis=0, keepdims=True)
    slots = lax.broadcasted_iota(jnp.int32, (128, CAP), 1).astype(F32)
    for e in range(EXPERTS):
        line = [ltall[b, e:e + 1, c * 128:(c + 1) * 128] for b in range(EP) for c in range(BLK // 128)]
        for c in range(BLK // 128):
            part = slice(c * 128, (c + 1) * 128)
            col = column(scores[e:e + 1, part])
            count = jnp.zeros((128, 128), F32)
            for piece in line:
                count = count + jnp.where(piece > col, 1.0, 0.0)
            rank = jnp.sum(count, axis=1, keepdims=True)
            back[e, part, :] = jnp.where(slots == rank, 1.0, 0.0).astype(BF16)
            gate[e, part, :] = column(probs[e:e + 1, part])

    def emit(j):
        copy_res(j, tp).start()
        store_res(j).start()

    for j in range(NJ + 2):
        if j < NJ:
            copy_s(j).wait_recv()
            for e in range(OWN):
                mine = acc[e, :, j * NC:(j + 1) * NC] + rcv[j, e * CAP:(e + 1) * CAP, :]
                zall[j, pl.ds(pl.multiple_of(ep * (OWN * CAP) + e * CAP, CAP), CAP), :] = mine.astype(BF16)
            copy_zx(j, ep).start()
            copy_zc(j, ep).start()
        if 0 <= j - 1 < NJ:
            copy_zx(j - 1, far).wait_recv()
            copy_zf(j - 1, far).start()
        if 0 <= j - 2 < NJ:
            copy_zc(j - 2, near).wait_recv()
            copy_zf(j - 2, diag).wait_recv()
            total = jnp.zeros((BLK, NC), F32)
            i = j - 2
            for e in range(EXPERTS):
                z = jnp.dot(back[e], zall[i, e * CAP:(e + 1) * CAP, :], preferred_element_type=F32)
                total = total + gate[e] * z
            base = i * NC
            own = xall[tp * (NK // 2) + base // KC, rows(ep), base % KC:base % KC + NC]
            res[i] = (own.astype(F32) + total).astype(BF16)
            emit(i)

    for i, where in enumerate((to_near, to_far, to_diag)):
        copy_lt(i, where, ep).wait_send()
    for k in range(NK):
        copy_a(k, ep).wait_send()
        copy_b(k, ep).wait_send()
        copy_c(k, far).wait_send()
        copy_d(k, tp).wait_send()
        copy_e(k, far).wait_send()
    for j in range(NJ):
        copy_s(j).wait_send()
        copy_zc(j, ep).wait_send()
        copy_zx(j, ep).wait_send()
        copy_zf(j, far).wait_send()
        copy_res(j, tp).wait_send()
        store_res(j).wait()
    for j in range(NJ):
        copy_res(j, peer).wait_recv()


def solution(mesh):
    def local_layer(tokens, logits, w_in, w_out):
        dma = pltpu.SemaphoreType.DMA
        scratch = [
            pltpu.VMEM((NK, TOK, KC), BF16),
            pltpu.VMEM((EP, EXPERTS, BLK), F32),
            pltpu.VMEM((OWN, CAP, TOK), BF16),
            pltpu.VMEM((CAP, KC), BF16),
            pltpu.VMEM((OWN, DIM, HID), BF16),
            pltpu.VMEM((OWN, CAP, HID), F32),
            pltpu.VMEM((OWN, CAP, HID), BF16),
            pltpu.VMEM((NB, OWN, HID, 2 * NC), BF16),
            pltpu.VMEM((NJ, OWN * CAP, NC), F32),
            pltpu.VMEM((NJ, OWN * CAP, NC), F32),
            pltpu.VMEM((NJ, EXPERTS * CAP, NC), BF16),
            pltpu.VMEM((EXPERTS, BLK, CAP), BF16),
            pltpu.VMEM((EXPERTS, BLK, NC), F32),
            pltpu.VMEM((NJ, BLK, NC), BF16),
            dma((NK,)), dma((OWN * NK,)), dma((NB, 4)), dma((NJ,)),
            dma((3,)), dma((3,)),
        ] + [dma((NK,))] * 10 + [dma((NJ,))] * 10
        return pl.pallas_call(
            kernel,
            out_shape=jax.ShapeDtypeStruct(tokens.shape, BF16),
            in_specs=[pl.BlockSpec(memory_space=pl.ANY), pl.BlockSpec(memory_space=pltpu.VMEM),
                      pl.BlockSpec(memory_space=pl.ANY), pl.BlockSpec(memory_space=pl.ANY)],
            out_specs=pl.BlockSpec(memory_space=pl.ANY),
            scratch_shapes=scratch,
            compiler_params=pltpu.CompilerParams(collective_id=0, has_side_effects=True,
                                                 vmem_limit_bytes=67_000_000),
            name="moe_layer",
        )(tokens, logits.T, w_in, w_out)

    row_spec = P(("dp", "ep"), None)
    return jax.shard_map(local_layer, mesh=mesh,
                         in_specs=(row_spec, row_spec, P("ep", None, "tp"), P("ep", "tp", None)),
                         out_specs=row_spec, check_vma=False)
```

```python
import jax
import jax.numpy as jnp
from jax import lax
from jax.experimental import pallas as pl
from jax.experimental.pallas import tpu as pltpu
from jax.sharding import PartitionSpec as P

MESH = pl.DeviceIdType.MESH
F32 = jnp.float32
BF16 = jnp.bfloat16

BLK = 256
HB = BLK // 2
EXPERTS = 8
OWN = 2
CAP = 256
HC = CAP // 2
DIM = 2048
HID = 2816
EP = 4
TOK = BLK * EP
HALF = DIM // 2
NQ = 4
KQ = DIM // NQ
NK = 8
KK = DIM // NK
NJ = 8
NC = HALF // NJ
NB = 3
TILE = 256
LAG = 4


def gelu(v):
    return 0.5 * v * (1.0 + jnp.tanh(v * (0.7978845608028654 + 0.035677408136300125 * (v * v))))


def column(row):
    return jnp.transpose(jnp.broadcast_to(row, (128, 128)))


def kernel(tok, lt, w_in, w_out, out,
           xall, ltall, slots, hot1, hot2, xg, win, acc, hid, wout, snd, mine, rcv, zall, back, gate, probs, res,
           loc_sem, win_sem, wout_sem, out_sem,
           lt_s, lt_r, sl_s, sl_r, a_s, a_r, b_s, b_r, c_s, c_r, d_s, d_r, e_s, e_r, f_s, f_r, g_s, g_r,
           s_s, s_r, zc_s, zc_r, zx_s, zx_r, zf_s, zf_r, res_s, res_r):
    scope = jax.named_scope
    ep = lax.axis_index("ep")
    tp = lax.axis_index("tp")
    core = lax.rem(ep, 2)
    chip = ep // 2
    near = ep + 1 - 2 * core
    far = lax.rem(ep + 2, 4)
    diag = 3 - ep
    peer = 1 - tp
    to_near, to_far, to_diag = {"ep": near, "tp": tp}, {"ep": far, "tp": tp}, {"ep": diag, "tp": tp}
    to_peer = {"ep": ep, "tp": peer}
    A, B = 2, 3
    place_near, place_far, place_diag = 1 - core, 2 + core, 3 - core

    def rows(place, half=None):
        if half is None:
            return pl.ds(pl.multiple_of(place * BLK, BLK), BLK)
        return pl.ds(pl.multiple_of(place * BLK + half * HB, HB), HB)

    def remote(src, dst, send, recv, where):
        return pltpu.make_async_remote_copy(src_ref=src, dst_ref=dst, send_sem=send, recv_sem=recv,
                                            device_id=where, device_id_type=MESH)

    def load_tok(q):
        return pltpu.make_async_copy(tok.at[:, pl.ds(q * KQ, KQ)], xall.at[q, rows(core)], loc_sem.at[q])

    def load_win(e, q):
        part = pl.ds(q * KQ, KQ)
        return pltpu.make_async_copy(w_in.at[e, part], win.at[e, part], win_sem.at[e * NQ + q])

    def load_wout(n, e, side):
        half = peer if side == 0 else tp
        cols = pl.ds(pl.multiple_of(half * HALF + (n % NJ) * NC, NC), NC)
        return pltpu.make_async_copy(w_out.at[e, :, cols], wout.at[n % NB, e, :, pl.ds(side * NC, NC)],
                                     wout_sem.at[n % NB, 2 * e + side])

    def piece(k, r):
        return xall.at[k // 2, r, pl.ds((k % 2) * KK, KK)]

    def copy_lt(i, where, place):
        return remote(lt, ltall.at[place], lt_s.at[i], lt_r.at[i], where)

    def copy_slots(i, where, place):
        return remote(slots.at[core], slots.at[place], sl_s.at[i], sl_r.at[i], where)

    def copy_a(k, place):
        return remote(piece(k, rows(place)), piece(k, rows(place)), a_s.at[k], a_r.at[k], to_near)

    def copy_b(k):
        return remote(piece(k, rows(core, tp)), piece(k, rows(A, tp)), b_s.at[k], b_r.at[k], to_far)

    def copy_c(k):
        return remote(piece(k, rows(A, tp)), piece(k, rows(A, tp)), c_s.at[k], c_r.at[k], to_near)

    def copy_d(k, half):
        return remote(piece(k, rows(A, half)), piece(k, rows(A, half)), d_s.at[k], d_r.at[k], to_peer)

    def copy_e(k):
        return remote(piece(k, rows(A, peer)), piece(k, rows(A, peer)), e_s.at[k], e_r.at[k], to_near)

    def copy_g(q):
        return remote(xall.at[q, rows(core)], xall.at[q, rows(B)], g_s.at[q], g_r.at[q], to_far)

    def copy_f(q):
        return remote(xall.at[q, rows(B)], xall.at[q, rows(B)], f_s.at[q], f_r.at[q], to_near)

    def copy_s(n):
        return remote(snd.at[n], rcv.at[n], s_s.at[n], s_r.at[n], to_peer)

    def copy_zc(n, place):
        return remote(zall.at[n, place], zall.at[n, place], zc_s.at[n], zc_r.at[n], to_near)

    def copy_zx(n, src, dst):
        return remote(zall.at[n, src], zall.at[n, dst], zx_s.at[n], zx_r.at[n], to_far)

    def copy_zf(n, place):
        return remote(zall.at[n, place], zall.at[n, place], zf_s.at[n], zf_r.at[n], to_near)

    def out_cols(half, j):
        return out.at[:, pl.ds(pl.multiple_of(half * HALF + j * NC, NC), NC)]

    def copy_res(j, half):
        return remote(res.at[j], out_cols(half, j), res_s.at[j], res_r.at[j], to_peer)

    def store_res(j):
        return pltpu.make_async_copy(res.at[j], out_cols(tp, j), out_sem.at[j])

    for q in range(NQ):
        load_tok(q).start()
    barrier = pltpu.get_barrier_semaphore()
    for where in (to_near, to_far, to_diag, to_peer):
        pl.semaphore_signal(barrier, inc=1, device_id=where, device_id_type=MESH)
    for q in range(NQ):
        load_tok(q).wait()
    for q in range(NQ):
        for e in range(OWN):
            load_win(e, q).start()
    for n in range(NB):
        for e in range(OWN):
            for side in range(2):
                load_wout(n, e, side).start()
    with scope("barrier"):
        pl.semaphore_wait(barrier, 4)

    copy_lt(0, to_near, core).start()
    copy_lt(1, to_far, 2 + core).start()
    copy_lt(2, to_diag, 2 + core).start()
    for k in range(NK):
        @pl.when(core == 0)
        def _():
            copy_b(k).start()
        copy_a(k, core).start()

    scores = lt[...]
    grown = jnp.exp(scores - jnp.max(scores, axis=0, keepdims=True))
    probs[...] = grown / jnp.sum(grown, axis=0, keepdims=True)
    ltall[core] = scores

    with scope("ltwait"):
        copy_lt(0, to_near, place_near).wait_recv()
        copy_lt(1, to_far, place_far).wait_recv()
        copy_lt(2, to_diag, place_diag).wait_recv()

    below = jnp.where(lax.broadcasted_iota(jnp.int32, (128, 128), 0) < lax.broadcasted_iota(jnp.int32, (128, 128), 1),
                      1.0, 0.0).astype(BF16)
    before = jnp.where(lax.broadcasted_iota(jnp.int32, (8, 8), 1) < lax.broadcasted_iota(jnp.int32, (8, 8), 0),
                       1.0, 0.0).astype(BF16)

    def pick(i):
        expert = ep * OWN + i
        line = jnp.concatenate([ltall[p, pl.ds(expert, 1), :] for p in range(EP)], axis=1)
        rank = jnp.zeros((1, TOK), F32)
        for s in range(TOK // 128):
            wide = jnp.concatenate([column(line[:, s * 128:(s + 1) * 128])] * (TOK // 128), axis=1)
            rank = rank + jnp.sum(jnp.where(wide > line, 1.0, 0.0), axis=0, keepdims=True)
        taken = jnp.where(rank < CAP, 1.0, 0.0)
        grid = jnp.concatenate([taken[:, s * 128:(s + 1) * 128] for s in range(8)], axis=0)
        grid16 = grid.astype(BF16)
        inside = jnp.dot(grid16, below, preferred_element_type=F32)
        ahead = jnp.sum(jnp.dot(before, grid16, preferred_element_type=F32), axis=1, keepdims=True)
        slot = jnp.where(grid > 0.5, inside + ahead, -1.0)
        slot = jnp.concatenate([slot[s:s + 1, :] for s in range(8)], axis=1)
        first_half = lax.broadcasted_iota(jnp.int32, (HC, TOK), 0).astype(F32)
        hot1[i * HC:(i + 1) * HC, :] = jnp.where(first_half[:, :3 * BLK] == slot[:, :3 * BLK], 1.0, 0.0).astype(BF16)
        hot2[i * HC:(i + 1) * HC, :] = jnp.where(first_half + HC == slot, 1.0, 0.0).astype(BF16)
        return slot

    with scope("pick"):
        slot_rows = [pick(i) for i in range(OWN)]
        slots[core] = jnp.concatenate(slot_rows + [jnp.zeros((8 - OWN, TOK), F32)], axis=0)

    def first(h, q):
        hot, depth = (hot1, 3 * BLK) if h == 0 else (hot2, TOK)
        xg[...] = jnp.dot(hot[...], xall[q, :depth, :], preferred_element_type=F32).astype(BF16)

        def body(e, _):
            if h == 0:
                load_win(e, q).wait()
            mid = pl.ds(pl.multiple_of(e * HC, HC), HC)
            for n in range(HID // TILE):
                cols = slice(n * TILE, (n + 1) * TILE)
                r = jnp.dot(xg[mid, :], win[e, q * KQ:(q + 1) * KQ, cols], preferred_element_type=F32)
                if q > 0:
                    r = r + acc[e, :, cols]
                if q < NQ - 1:
                    acc[e, :, cols] = r
                else:
                    hid[h, e, :, cols] = gelu(r).astype(BF16)
            return 0
        lax.fori_loop(0, OWN, body, 0)

    def second(h, j):
        n = h * NJ + j

        def body(e, _):
            for side in range(2):
                load_wout(n, e, side).wait()
            r = jnp.dot(hid[h, e], wout[n % NB, e], preferred_element_type=F32)
            mid = pl.ds(pl.multiple_of(e * HC, HC), HC)
            snd[n, mid, :] = r[:, :NC]
            mine[n, mid, :] = r[:, NC:]
            return 0
        lax.fori_loop(0, OWN, body, 0)
        copy_s(n).start()
        if n + NB < 2 * NJ:
            for e in range(OWN):
                for side in range(2):
                    load_wout(n + NB, e, side).start()

    def relay_d(k):
        @pl.when(core == 0)
        def _():
            copy_d(k, peer).wait_recv()
            copy_e(k).start()

    for k in range(NK):
        with scope(f"relay{k}"):
            @pl.when(core == 0)
            def _():
                copy_b(k).wait_recv()
                copy_c(k).start()
                copy_d(k, tp).start()

            @pl.when(core == 1)
            def _():
                copy_c(k).wait_recv()
                if k == NK - 2:
                    for q in range(NQ):
                        copy_g(q).start()
            if k >= LAG:
                relay_d(k - LAG)

    copy_slots(0, to_near, core).start()
    copy_slots(1, to_far, 2 + core).start()
    copy_slots(2, to_diag, 2 + core).start()

    for q in range(NQ):
        with scope(f"arrive{q}"):
            if q == 2:
                relay_d(NK - 2)
                relay_d(NK - 1)
            elif q < 2:
                relay_d(NK - LAG + q)
            for k in (2 * q, 2 * q + 1):
                copy_a(k, place_near).wait_recv()

                @pl.when(core == 1)
                def _():
                    copy_e(k).wait_recv()
        with scope(f"first{q}"):
            first(0, q)

    def relay_g(q):
        @pl.when(core == 1)
        def _():
            copy_g(q).wait_recv()
            copy_f(q).start()

    relays = {1: 0, 4: 1, 7: 2}
    for j in range(NJ):
        with scope(f"second{j}"):
            second(0, j)
        if j in relays:
            with scope(f"relayg{relays[j]}"):
                relay_g(relays[j])

    for q in range(NQ):
        with scope(f"arriveB{q}"):
            if q == 1:
                relay_g(3)

            @pl.when(core == 0)
            def _():
                copy_f(q).wait_recv()
        with scope(f"firstB{q}"):
            first(1, q)
    for j in range(NJ):
        with scope(f"secondB{j}"):
            second(1, j)

    with scope("slotwait"):
        copy_slots(0, to_near, place_near).wait_recv()
        copy_slots(1, to_far, place_far).wait_recv()
        copy_slots(2, to_diag, place_diag).wait_recv()
    with scope("back"):
        lanes = lax.broadcasted_iota(jnp.int32, (128, CAP), 1).astype(F32)
        for p in range(EP):
            mark = core if p < 2 else 2 + core
            owner = lax.rem(2 * chip + p, 4)
            for i in range(OWN):
                for c in range(BLK // 128):
                    part = slice(c * 128, (c + 1) * 128)
                    here = pl.ds(pl.multiple_of(mark * BLK + c * 128, 128), 128)
                    col = column(slots[p, i:i + 1, here])
                    back[p * OWN + i, part, :] = jnp.where(jnp.concatenate([col, col], axis=1) == lanes, 1.0, 0.0).astype(BF16)
                    gate[p * OWN + i, part, :] = column(probs[pl.ds(owner * OWN + i, 1), :][:, part])

    def close(n):
        with scope(f"waits{n}"):
            copy_s(n).wait_recv()
        zall[n, core] = (mine[n] + rcv[n]).astype(BF16)
        copy_zx(n, core, 2 + core).start()
        copy_zc(n, core).start()

    def forward(n):
        with scope(f"waitzx{n}"):
            copy_zx(n, place_far, place_far).wait_recv()
        copy_zf(n, place_far).start()

    def landed(n):
        with scope(f"waitzf{n}"):
            copy_zc(n, place_near).wait_recv()
            copy_zf(n, place_diag).wait_recv()

    def combine(j):
        total = jnp.zeros((BLK, NC), F32)
        for p in range(EP):
            for i in range(OWN):
                mid = slice(i * HC, (i + 1) * HC)
                z = jnp.concatenate([zall[j, p, mid, :], zall[NJ + j, p, mid, :]], axis=0)
                total = total + gate[p * OWN + i] * jnp.dot(back[p * OWN + i], z, preferred_element_type=F32)
        base = j * NC
        own = xall[tp * (NQ // 2) + base // KQ, rows(core), base % KQ:base % KQ + NC]
        res[j] = (own.astype(F32) + total).astype(BF16)
        copy_res(j, tp).start()
        store_res(j).start()

    for n in range(2 * NJ + 2):
        if n < 2 * NJ:
            close(n)
        if 0 <= n - 1 < 2 * NJ:
            forward(n - 1)
        if 0 <= n - 2:
            landed(n - 2)
            if n - 2 >= NJ:
                combine(n - 2 - NJ)

    with scope("drain"):
        for i, where in enumerate((to_near, to_far, to_diag)):
            copy_lt(i, where, core).wait_send()
            copy_slots(i, where, core).wait_send()
        for k in range(NK):
            copy_a(k, core).wait_send()

            @pl.when(core == 0)
            def _():
                copy_b(k).wait_send()
                copy_c(k).wait_send()
                copy_d(k, tp).wait_send()
                copy_e(k).wait_send()

        @pl.when(core == 1)
        def _():
            for q in range(NQ):
                copy_g(q).wait_send()
                copy_f(q).wait_send()
        for n in range(2 * NJ):
            copy_s(n).wait_send()
            copy_zc(n, core).wait_send()
            copy_zx(n, core, place_far).wait_send()
            copy_zf(n, place_far).wait_send()
        for j in range(NJ):
            copy_res(j, tp).wait_send()
            store_res(j).wait()
        for j in range(NJ):
            copy_res(j, peer).wait_recv()


def solution(mesh):
    def local_layer(tokens, logits, w_in, w_out):
        dma = pltpu.SemaphoreType.DMA
        scratch = [
            pltpu.VMEM((NQ, TOK, KQ), BF16),
            pltpu.VMEM((EP, EXPERTS, BLK), F32),
            pltpu.VMEM((EP, 8, TOK), F32),
            pltpu.VMEM((OWN * HC, 3 * BLK), BF16),
            pltpu.VMEM((OWN * HC, TOK), BF16),
            pltpu.VMEM((OWN * HC, KQ), BF16),
            pltpu.VMEM((OWN, DIM, HID), BF16),
            pltpu.VMEM((OWN, HC, HID), F32),
            pltpu.VMEM((2, OWN, HC, HID), BF16),
            pltpu.VMEM((NB, OWN, HID, 2 * NC), BF16),
            pltpu.VMEM((2 * NJ, OWN * HC, NC), F32),
            pltpu.VMEM((2 * NJ, OWN * HC, NC), F32),
            pltpu.VMEM((2 * NJ, OWN * HC, NC), F32),
            pltpu.VMEM((2 * NJ, EP, OWN * HC, NC), BF16),
            pltpu.VMEM((EXPERTS, BLK, CAP), BF16),
            pltpu.VMEM((EXPERTS, BLK, NC), F32),
            pltpu.VMEM((EXPERTS, BLK), F32),
            pltpu.VMEM((NJ, BLK, NC), BF16),
            dma((NQ,)), dma((OWN * NQ,)), dma((NB, 4)), dma((NJ,)),
            dma((3,)), dma((3,)), dma((3,)), dma((3,)),
        ] + [dma((NK,))] * 10 + [dma((NQ,))] * 4 + [dma((2 * NJ,))] * 8 + [dma((NJ,))] * 2
        return pl.pallas_call(
            kernel,
            out_shape=jax.ShapeDtypeStruct(tokens.shape, BF16),
            in_specs=[pl.BlockSpec(memory_space=pl.ANY), pl.BlockSpec(memory_space=pltpu.VMEM),
                      pl.BlockSpec(memory_space=pl.ANY), pl.BlockSpec(memory_space=pl.ANY)],
            out_specs=pl.BlockSpec(memory_space=pl.ANY),
            scratch_shapes=scratch,
            compiler_params=pltpu.CompilerParams(collective_id=0, has_side_effects=True,
                                                 vmem_limit_bytes=67_000_000),
            name="moe_layer",
        )(tokens, logits.T, w_in, w_out)

    row_spec = P(("dp", "ep"), None)
    return jax.shard_map(local_layer, mesh=mesh,
                         in_specs=(row_spec, row_spec, P("ep", None, "tp"), P("ep", "tp", None)),
                         out_specs=row_spec, check_vma=False)
```

```python
import jax
import jax.numpy as jnp
from jax import lax
from jax.experimental import pallas as pl
from jax.experimental.pallas import tpu as pltpu
from jax.sharding import PartitionSpec as P

MESH = pl.DeviceIdType.MESH
F32 = jnp.float32
BF16 = jnp.bfloat16

BLK = 256
XR = 128
YR = BLK - XR
EXPERTS = 8
OWN = 2
CAP = 256
HC = CAP // 2
DIM = 2048
HID = 2816
EP = 4
TOK = BLK * EP
HALF = DIM // 2
NK = 8
KK = DIM // NK
NG = 4
KG = DIM // NG
NJ = 8
NC = HALF // NJ
GRP = 4
NB = 6
TILE = 256
EARLY = 2


def gelu(v):
    return 0.5 * v * (1.0 + jnp.tanh(v * (0.7978845608028654 + 0.035677408136300125 * (v * v))))


def column(row):
    return jnp.transpose(jnp.broadcast_to(row, (128, 128)))


def kernel(tok, lt, w_in, w_out, out,
           xall, ltall, slots, hot1, hot2, xg, xg2, win, acc, hid, wout, snd, mine, rcv, zall, back, gate, probs, res,
           local_sem, win_sem, wout_sem, send, lt_r, sl_r, a_r, bc_r, de_r, gf_r, s_r, zx_r, zn_r, res_r):
    scope = jax.named_scope
    ep = lax.axis_index("ep")
    tp = lax.axis_index("tp")
    core = lax.rem(ep, 2)
    chip = ep // 2
    near = ep + 1 - 2 * core
    far = lax.rem(ep + 2, 4)
    diag = 3 - ep
    peer = 1 - tp
    to_near, to_far, to_diag = {"ep": near, "tp": tp}, {"ep": far, "tp": tp}, {"ep": diag, "tp": tp}
    to_peer = {"ep": ep, "tp": peer}
    A, B = 2, 3
    place_near, place_far, place_diag = 1 - core, 3 - core, 2 + core
    there = 3 - core
    lead, follow = core == 1, core == 0

    def rows(place, offset=0, size=BLK):
        return pl.ds(pl.multiple_of(place * BLK + offset, 32), size)

    def remote(src, dst, family, recv, where):
        return pltpu.make_async_remote_copy(src_ref=src, dst_ref=dst, send_sem=send.at[family], recv_sem=recv,
                                            device_id=where, device_id_type=MESH)

    def load_tok(k):
        return pltpu.make_async_copy(tok.at[:, pl.ds(k * KK, KK)], xall.at[k, rows(core)], local_sem.at[0 if k < EARLY else 1])

    def load_win(e, g):
        part = pl.ds(g * KG, KG)
        return pltpu.make_async_copy(w_in.at[e, part], win.at[e, part], win_sem.at[g])

    def wait_win(g):
        both = win.at[:, pl.ds(g * KG, KG)]
        pltpu.make_async_copy(both, both, win_sem.at[g]).wait()

    head = [(0, 0, 0), (0, 1, 0)]
    order = head + [(0, 2, 0), (0, 3, 0)] + [(0, j, 1) for j in range(4)]
    order += [(0, j, e) for j in range(4, NJ) for e in range(OWN)] + [(1, j, e) for j in range(NJ) for e in range(OWN)]

    def load_wout(m):
        if m >= len(order):
            return
        _, j, e = order[m]
        for side, half in enumerate((peer, tp)):
            cols = pl.ds(pl.multiple_of(half * HALF + j * NC, NC), NC)
            pltpu.make_async_copy(w_out.at[e, :, cols], wout.at[m % NB, :, pl.ds(side * NC, NC)], wout_sem.at[m % NB]).start()

    def wait_wout(m):
        both = wout.at[m % NB]
        pltpu.make_async_copy(both, both, wout_sem.at[m % NB]).wait()

    def copy_lt(where, place):
        return remote(ltall.at[core], ltall.at[place], 0, lt_r.at[0], where)

    def copy_slots(where, place):
        return remote(slots.at[core], slots.at[place], 1, sl_r.at[0], where)

    def copy_a(k, place):
        return remote(xall.at[k, rows(place)], xall.at[k, rows(place)], 2, a_r.at[0], to_near)

    def copy_b(k):
        return remote(xall.at[k, rows(core, tp * YR, XR)], xall.at[k, rows(A, tp * YR, XR)], 3, bc_r.at[k], to_far)

    def copy_c(k):
        piece = xall.at[k, rows(A, tp * YR, XR)]
        return remote(piece, piece, 4, bc_r.at[k], to_near)

    def copy_d(k, half):
        piece = xall.at[k, rows(A, half * XR, YR)]
        return remote(piece, piece, 5, de_r.at[k], to_peer)

    def copy_e(k):
        piece = xall.at[k, rows(A, peer * XR, YR)]
        return remote(piece, piece, 6, de_r.at[k], to_near)

    def copy_g(g):
        pair = pl.ds(2 * g, 2)
        return remote(xall.at[pair, rows(core)], xall.at[pair, rows(B)], 7, gf_r.at[g], to_far)

    def copy_f(g):
        pair = xall.at[pl.ds(2 * g, 2), rows(B)]
        return remote(pair, pair, 8, gf_r.at[g], to_near)

    def span(u):
        return (GRP * u, GRP) if u < NJ // GRP else (NJ + u - NJ // GRP, 1)

    def unit(n):
        return n // GRP if n < NJ else NJ // GRP + n - NJ

    def copy_s(n, e):
        mid = pl.ds(e * HC, HC)
        return remote(snd.at[n, mid], rcv.at[n, mid], 9, s_r.at[unit(n)], to_peer)

    def wait_s(u):
        whole = rcv.at[pl.ds(*span(u))]
        remote(whole, whole, 9, s_r.at[u], to_peer).wait_recv()

    def copy_zc(u, place):
        part = zall.at[pl.ds(*span(u)), place]
        return remote(part, part, 10, zn_r.at[max(0, u - NJ // GRP + 1)], to_near)

    def copy_zf(u, place):
        part = zall.at[pl.ds(*span(u)), place]
        return remote(part, part, 11, zn_r.at[max(0, u - NJ // GRP + 1)], to_near)

    def wait_zn(j):
        whole = zall.at[pl.ds(0, NJ), pl.ds(0, 2)] if j < 0 else zall.at[NJ + j, pl.ds(0, 2)]
        remote(whole, whole, 10, zn_r.at[j + 1], to_near).wait_recv()

    def copy_zx(u, src, dst):
        ns = pl.ds(*span(u))
        return remote(zall.at[ns, src], zall.at[ns, dst], 12, zx_r.at[u], to_far)

    def out_cols(half, j):
        return out.at[:, pl.ds(pl.multiple_of(half * HALF + j * NC, NC), NC)]

    def copy_res(j, half):
        return remote(res.at[j], out_cols(half, j), 13, res_r.at[0], to_peer)

    barrier = pltpu.get_barrier_semaphore()
    for where in (to_near, to_far, to_diag, to_peer):
        pl.semaphore_signal(barrier, inc=1, device_id=where, device_id_type=MESH)
    load_lt = pltpu.make_async_copy(lt, ltall.at[core], local_sem.at[2])
    load_lt.start()
    for k in range(NK):
        load_tok(k).start()
    mine_x = xall.at[:, rows(core)]
    load_lt.wait()
    early, late = (xall.at[pl.ds(a, n), rows(core)] for a, n in ((0, EARLY), (EARLY, NK - EARLY)))
    pltpu.make_async_copy(early, early, local_sem.at[0]).wait()
    with scope("barrier"):
        pl.semaphore_wait(barrier, 4)

    def send_pieces(ks):
        @pl.when(lead)
        def _():
            for k in ks:
                copy_b(k).start()
        for k in ks:
            copy_a(k, core).start()

    copy_lt(to_near, core).start()
    copy_lt(to_far, there).start()
    copy_lt(to_diag, there).start()
    send_pieces(range(EARLY))
    pltpu.make_async_copy(late, late, local_sem.at[1]).wait()
    send_pieces(range(EARLY, NK))
    for g in range(NG):
        for e in range(OWN):
            load_win(e, g).start()
    for m in range(NB):
        load_wout(m)

    scores = ltall[core]
    grown = jnp.exp(scores - jnp.max(scores, axis=0, keepdims=True))
    probs[...] = grown / jnp.sum(grown, axis=0, keepdims=True)

    with scope("ltwait"):
        three = ltall.at[pl.ds(0, 3)]
        remote(three, three, 0, lt_r.at[0], to_near).wait_recv()

    below = jnp.where(lax.broadcasted_iota(jnp.int32, (128, 128), 0) < lax.broadcasted_iota(jnp.int32, (128, 128), 1),
                      1.0, 0.0).astype(BF16)
    before = jnp.where(lax.broadcasted_iota(jnp.int32, (8, 8), 1) < lax.broadcasted_iota(jnp.int32, (8, 8), 0),
                       1.0, 0.0).astype(BF16)

    first_half = lax.broadcasted_iota(jnp.int32, (HC, TOK), 0).astype(F32)

    def pick(i):
        expert = ep * OWN + i
        line = jnp.concatenate([ltall[p, pl.ds(expert, 1), :] for p in range(EP)], axis=1)
        rank = jnp.zeros((1, TOK), F32)
        for s in range(TOK // 128):
            wide = jnp.concatenate([column(line[:, s * 128:(s + 1) * 128])] * (TOK // 128), axis=1)
            rank = rank + jnp.sum(jnp.where(wide > line, 1.0, 0.0), axis=0, keepdims=True)
        taken = jnp.where(rank < CAP, 1.0, 0.0)
        grid = jnp.concatenate([taken[:, s * 128:(s + 1) * 128] for s in range(8)], axis=0)
        grid16 = grid.astype(BF16)
        inside = jnp.dot(grid16, below, preferred_element_type=F32)
        ahead = jnp.sum(jnp.dot(before, grid16, preferred_element_type=F32), axis=1, keepdims=True)
        slot = jnp.where(grid > 0.5, inside + ahead, -1.0)
        slots[core, i * 8:(i + 1) * 8, :] = slot
        slot = jnp.concatenate([slot[s:s + 1, :] for s in range(8)], axis=1)
        hot1[i * HC:(i + 1) * HC, :] = jnp.where(first_half[:, :3 * BLK] == slot[:, :3 * BLK], 1.0, 0.0).astype(BF16)

    def pick_late():
        for i in range(OWN):
            slot = jnp.concatenate([slots[core, i * 8 + s:i * 8 + s + 1, :] for s in range(8)], axis=1)
            hot2[i * HC:(i + 1) * HC, :] = jnp.where(first_half + HC == slot, 1.0, 0.0).astype(BF16)

    def take_own(ks):
        for k in ks:
            xg[k] = jnp.dot(hot1[:, :2 * BLK], xall[k, :2 * BLK, :], preferred_element_type=F32).astype(BF16)

    def take_a(ks):
        for k in ks:
            r = jnp.dot(hot1[:, 2 * BLK:], xall[k, A * BLK:(A + 1) * BLK, :], preferred_element_type=F32)
            xg[k] = (xg[k].astype(F32) + r).astype(BF16)

    def first_tiles(h, g, e, x):
        for n in range(HID // TILE):
            cols = slice(n * TILE, (n + 1) * TILE)
            r = jnp.dot(x, win[e, g * KG:(g + 1) * KG, cols], preferred_element_type=F32)
            if g > 0:
                r = r + acc[e, :, cols]
            if g < NG - 1:
                acc[e, :, cols] = r
            else:
                hid[h, e, :, cols] = gelu(r).astype(BF16)

    def first(g, e):
        with scope(f"first{g}e{e}"):
            if e == 0:
                wait_win(g)
                take_a((2 * g, 2 * g + 1))
            mid = slice(e * HC, (e + 1) * HC)
            first_tiles(0, g, e, jnp.concatenate([xg[2 * g, mid, :], xg[2 * g + 1, mid, :]], axis=1))

    def first_late(g):
        for m in range(2):
            xg2[:, m * KK:(m + 1) * KK] = jnp.dot(hot2[...], xall[2 * g + m], preferred_element_type=F32).astype(BF16)

        def body(e, _):
            first_tiles(1, g, e, xg2[pl.ds(pl.multiple_of(e * HC, HC), HC), :])
            return 0
        lax.fori_loop(0, OWN, body, 0)

    def second(m):
        h, j, e = order[m]
        n = h * NJ + j
        with scope(f"second{n}e{e}"):
            wait_wout(m)
            r = jnp.dot(hid[h, e], wout[m % NB], preferred_element_type=F32)
            mid = slice(e * HC, (e + 1) * HC)
            snd[n, mid, :] = r[:, :NC]
            mine[n, mid, :] = r[:, NC:]
            copy_s(n, e).start()
            load_wout(m + NB)

    def relay_b(*ks):
        for k in ks:
            with scope(f"relayb{k}"):
                @pl.when(lead)
                def _():
                    copy_b(k).wait_recv()
                    copy_c(k).start()
                    copy_d(k, tp).start()

    def relay_d(*ks):
        for k in ks:
            with scope(f"relayd{k}"):
                @pl.when(lead)
                def _():
                    copy_d(k, peer).wait_recv()
                    copy_e(k).start()

    def ready(*ks):
        with scope(f"ready{ks[0]}"):
            @pl.when(follow)
            def _():
                for k in ks:
                    copy_c(k).wait_recv()
                    if k == NK - 2:
                        for g in range(NG):
                            copy_g(g).start()
                    copy_e(k).wait_recv()

    relay_b(0)
    with scope("pick0"):
        pick(0)
    relay_b(1)
    with scope("pick1"):
        pick(1)
    relay_b(2, 3)
    with scope("wait_a"):
        near_x = xall.at[:, rows(place_near)]
        remote(near_x, near_x, 2, a_r.at[0], to_near).wait_recv()
    with scope("own0"):
        take_own(range(4))
    relay_b(4)
    relay_d(0)
    with scope("own1"):
        take_own(range(4, NK))
    relay_b(5)
    relay_d(1)
    ready(0, 1)
    first(0, 0)
    relay_b(6)
    relay_d(2, 3)
    ready(2, 3)
    first(1, 0)
    relay_b(7)
    relay_d(4)
    first(0, 1)
    relay_d(5)
    ready(4, 5)
    first(2, 0)
    relay_d(6)
    first(1, 1)
    relay_d(7)
    ready(6, 7)
    first(3, 0)
    for m in range(len(head)):
        second(m)
    first(2, 1)
    first(3, 1)
    copy_slots(to_near, core).start()
    copy_slots(to_far, there).start()
    copy_slots(to_diag, there).start()

    def relay_g(g):
        with scope(f"relayg{g}"):
            @pl.when(follow)
            def _():
                copy_g(g).wait_recv()
                copy_f(g).start()

    half = OWN * NJ
    for m in range(len(head), half):
        second(m)
        if m in (half - 8, half - 2):
            relay_g(0 if m == half - 8 else 1)
    with scope("pick_late"):
        pick_late()
    for g in range(NG):
        if g > 0 and g + 1 < NG:
            relay_g(g + 1)
        with scope(f"readyB{g}"):
            @pl.when(lead)
            def _():
                copy_f(g).wait_recv()
        with scope(f"firstB{g}"):
            first_late(g)
    for m in range(half, 2 * half):
        second(m)

    def close(u):
        with scope(f"waits{u}"):
            wait_s(u)
        start, size = span(u)
        for n in range(start, start + size):
            zall[n, core] = (mine[n] + rcv[n]).astype(BF16)
        copy_zx(u, core, there).start()
        copy_zc(u, core).start()

    def forward(u):
        with scope(f"waitzx{u}"):
            copy_zx(u, place_far, place_far).wait_recv()
        copy_zf(u, place_far).start()

    def combine(j):
        with scope(f"waitzn{j}"):
            if j == 0:
                wait_zn(-1)
            wait_zn(j)
        total = jnp.zeros((BLK, NC), F32)
        for p in range(EP):
            for i in range(OWN):
                mid = slice(i * HC, (i + 1) * HC)
                z = jnp.concatenate([zall[j, p, mid, :], zall[NJ + j, p, mid, :]], axis=0)
                total = total + gate[p * OWN + i] * jnp.dot(back[p * OWN + i], z, preferred_element_type=F32)
        per = KK // NC
        own = xall[tp * (NK // 2) + j // per, rows(core), (j % per) * NC:(j % per + 1) * NC]
        res[j] = (own.astype(F32) + total).astype(BF16)
        copy_res(j, tp).start()
        out[:, pl.ds(pl.multiple_of(tp * HALF + j * NC, NC), NC)] = res[j]

    close(0)

    with scope("slotwait"):
        three = slots.at[pl.ds(0, 3)]
        remote(three, three, 1, sl_r.at[0], to_near).wait_recv()
    with scope("back"):
        lanes = lax.broadcasted_iota(jnp.int32, (128, CAP), 1).astype(F32)
        for p in range(EP):
            mark = core if p < 2 else there
            owner = 2 * chip + p if p < 2 else 2 * (1 - chip) + (3 - p)
            for i in range(OWN):
                for c in range(BLK // 128):
                    part = slice(c * 128, (c + 1) * 128)
                    col = column(slots[p, pl.ds(i * 8 + mark * 2 + c, 1), :])
                    back[p * OWN + i, part, :] = jnp.where(jnp.concatenate([col, col], axis=1) == lanes, 1.0, 0.0).astype(BF16)
                    gate[p * OWN + i, part, :] = column(probs[pl.ds(owner * OWN + i, 1), :][:, part])

    first_units = NJ // GRP
    units = first_units + NJ
    for u in range(1, units + 2):
        if u < units:
            close(u)
        if u - 1 < units:
            forward(u - 1)
        if u - 2 >= first_units:
            combine(u - 2 - first_units)

    with scope("drain"):
        def left(ref, family):
            remote(ref, ref, family, res_r.at[0], to_near).wait_send()
        left(ltall.at[pl.ds(0, 3)], 0)
        left(slots.at[pl.ds(0, 3)], 1)
        left(mine_x, 2)

        @pl.when(lead)
        def _():
            left(xall.at[:, rows(A, 0, XR)], 3)
            left(xall.at[:, rows(A, 0, XR)], 4)
            left(xall.at[:, rows(A, 0, YR)], 5)
            left(xall.at[:, rows(A, 0, YR)], 6)

        @pl.when(follow)
        def _():
            left(mine_x, 7)
            left(mine_x, 8)
        left(snd, 9)
        for family in (10, 11, 12):
            left(zall.at[:, 0], family)
        left(res, 13)
        remote(res, res, 13, res_r.at[0], to_peer).wait_recv()


def solution(mesh):
    def local_layer(tokens, logits, w_in, w_out):
        dma = pltpu.SemaphoreType.DMA
        units = NJ // GRP + NJ
        scratch = [
            pltpu.VMEM((NK, TOK, KK), BF16),
            pltpu.VMEM((EP, EXPERTS, BLK), F32),
            pltpu.VMEM((EP, OWN * 8, 128), F32),
            pltpu.VMEM((OWN * HC, 3 * BLK), BF16),
            pltpu.VMEM((OWN * HC, TOK), BF16),
            pltpu.VMEM((NK, OWN * HC, KK), BF16),
            pltpu.VMEM((OWN * HC, 2 * KK), BF16),
            pltpu.VMEM((OWN, DIM, HID), BF16),
            pltpu.VMEM((OWN, HC, HID), F32),
            pltpu.VMEM((2, OWN, HC, HID), BF16),
            pltpu.VMEM((NB, HID, 2 * NC), BF16),
            pltpu.VMEM((2 * NJ, OWN * HC, NC), F32),
            pltpu.VMEM((2 * NJ, OWN * HC, NC), F32),
            pltpu.VMEM((2 * NJ, OWN * HC, NC), F32),
            pltpu.VMEM((2 * NJ, EP, OWN * HC, NC), BF16),
            pltpu.VMEM((EXPERTS, BLK, CAP), BF16),
            pltpu.VMEM((EXPERTS, BLK, NC), F32),
            pltpu.VMEM((EXPERTS, BLK), F32),
            pltpu.VMEM((NJ, BLK, NC), BF16),
            dma((3,)), dma((NG,)), dma((NB,)), dma((14,)),
            dma((1,)), dma((1,)), dma((1,)), dma((NK,)), dma((NK,)), dma((NG,)),
            dma((units,)), dma((units,)), dma((1 + NJ,)), dma((1,)),
        ]
        return pl.pallas_call(
            kernel,
            out_shape=pltpu.VMEM(tokens.shape, BF16),
            in_specs=[pl.BlockSpec(memory_space=pl.ANY), pl.BlockSpec(memory_space=pl.ANY),
                      pl.BlockSpec(memory_space=pl.ANY), pl.BlockSpec(memory_space=pl.ANY)],
            out_specs=pl.BlockSpec(memory_space=pltpu.VMEM),
            scratch_shapes=scratch,
            compiler_params=pltpu.CompilerParams(collective_id=0, has_side_effects=True,
                                                 vmem_limit_bytes=62_500_000),
            name="moe_layer",
        )(tokens, logits.T, w_in, w_out)

    row_spec = P(("dp", "ep"), None)
    return jax.shard_map(local_layer, mesh=mesh,
                         in_specs=(row_spec, row_spec, P("ep", None, "tp"), P("ep", "tp", None)),
                         out_specs=row_spec, check_vma=False)
```

```python
import jax
import jax.numpy as jnp
from jax import lax
from jax.experimental import pallas as pl
from jax.experimental.pallas import tpu as pltpu
from jax.sharding import PartitionSpec as P

MESH = pl.DeviceIdType.MESH
F32 = jnp.float32
BF16 = jnp.bfloat16

BLK = 256
XR = 128
YR = BLK - XR
EXPERTS = 8
OWN = 2
CAP = 256
HC = CAP // 2
DIM = 2048
HID = 2816
EP = 4
TOK = BLK * EP
HALF = DIM // 2
UNIT = 128
PIECES = [(0, 1), (1, 1)] + [(u, 2) for u in range(2, 12, 2)] + [(14, 1), (12, 2), (15, 1)]
TWO_WAY = 8
NP = len(PIECES)
NG = 4
KG = DIM // NG
UG = KG // UNIT
NJ = 8
NC = HALF // NJ
SPANS = [(0, 4), (4, 4), (8, 2), (10, 2), (12, 2), (14, 1), (15, 1)]
EARLY_SPANS = 2
NB = 6
TILE = 256
EARLY = 3
EARLY_UNITS = 4


def gelu(v):
    return 0.5 * v * (1.0 + jnp.tanh(v * (0.7978845608028654 + 0.035677408136300125 * (v * v))))


def column(row):
    return jnp.transpose(jnp.broadcast_to(row, (128, 128)))


def kernel(tok, lt, w_in, w_out, out,
           xall, ltall, slots, hot1, hot2, xg, xg2, win, acc, hid, wout, snd, mine, rcv, zall, back, gate, probs, res,
           local_sem, win_sem, wout_sem, send, lt_r, sl_r, a_r, bc_r, de_r, gf_r, s_r, zx_r, zn_r, res_r):
    scope = jax.named_scope
    ep = lax.axis_index("ep")
    tp = lax.axis_index("tp")
    core = lax.rem(ep, 2)
    chip = ep // 2
    near = ep + 1 - 2 * core
    far = lax.rem(ep + 2, 4)
    diag = 3 - ep
    peer = 1 - tp
    to_near, to_far, to_diag = {"ep": near, "tp": tp}, {"ep": far, "tp": tp}, {"ep": diag, "tp": tp}
    to_peer = {"ep": ep, "tp": peer}
    A, B = 2, 3
    place_near, place_far, place_diag = 1 - core, 3 - core, 2 + core
    there = 3 - core
    lead, follow = core == 1, core == 0

    def rows(place, offset=0, size=BLK):
        return pl.ds(pl.multiple_of(place * BLK + offset, 32), size)

    def remote(src, dst, family, recv, where):
        return pltpu.make_async_remote_copy(src_ref=src, dst_ref=dst, send_sem=send.at[family], recv_sem=recv,
                                            device_id=where, device_id_type=MESH)

    def load_tok(k):
        return pltpu.make_async_copy(tok.at[:, pl.ds(k * UNIT, UNIT)], xall.at[k, rows(core)], local_sem.at[0 if k < EARLY_UNITS else 1])

    def load_win(e, g):
        part = pl.ds(g * KG, KG)
        return pltpu.make_async_copy(w_in.at[e, part], win.at[e, part], win_sem.at[OWN * g + e])

    def wait_win(e, g):
        load_win(e, g).wait()

    head = [(0, 0, 0), (0, 1, 0), (0, 2, 0)]
    order = head + [(0, 3, 0)] + [(0, j, 1) for j in range(4)]
    order += [(0, j, e) for j in range(4, NJ) for e in range(OWN)] + [(1, j, e) for j in range(NJ) for e in range(OWN)]

    def load_wout(m):
        if m >= len(order):
            return
        _, j, e = order[m]
        for side, half in enumerate((peer, tp)):
            cols = pl.ds(pl.multiple_of(half * HALF + j * NC, NC), NC)
            pltpu.make_async_copy(w_out.at[e, :, cols], wout.at[m % NB, :, pl.ds(side * NC, NC)], wout_sem.at[m % NB]).start()

    def wait_wout(m):
        both = wout.at[m % NB]
        pltpu.make_async_copy(both, both, wout_sem.at[m % NB]).wait()

    def copy_lt(where, place):
        return remote(ltall.at[core], ltall.at[place], 0, lt_r.at[0], where)

    def copy_slots(where, place):
        return remote(slots.at[core], slots.at[place], 0, sl_r.at[0], where)

    def copy_a(k, place):
        piece = xall.at[pl.ds(*PIECES[k]), rows(place)]
        return remote(piece, piece, 1, a_r.at[0], to_near)

    def b_rows(k, place):
        return rows(place, tp * YR, XR) if k < TWO_WAY else rows(place)

    def copy_b(k):
        units = pl.ds(*PIECES[k])
        return remote(xall.at[units, b_rows(k, core)], xall.at[units, b_rows(k, A)], 1, bc_r.at[k], to_far)

    def copy_c(k):
        piece = xall.at[pl.ds(*PIECES[k]), b_rows(k, A)]
        return remote(piece, piece, 1, bc_r.at[k], to_near)

    def copy_d(k, half):
        piece = xall.at[pl.ds(*PIECES[k]), rows(A, half * XR, YR)]
        return remote(piece, piece, 1, de_r.at[k], to_peer)

    def copy_e(k):
        piece = xall.at[pl.ds(*PIECES[k]), rows(A, peer * XR, YR)]
        return remote(piece, piece, 1, de_r.at[k], to_near)

    def copy_g(g):
        group = pl.ds(UG * g, UG)
        return remote(xall.at[group, rows(core)], xall.at[group, rows(B)], 1, gf_r.at[g], to_far)

    def copy_f(g):
        group = xall.at[pl.ds(UG * g, UG), rows(B)]
        return remote(group, group, 1, gf_r.at[g], to_near)

    def span(u):
        return SPANS[u]

    def unit(n):
        return [u for u, (start, size) in enumerate(SPANS) if start <= n < start + size][0]

    def copy_s(n, e):
        mid = pl.ds(e * HC, HC)
        return remote(snd.at[n, mid], rcv.at[n, mid], 3, s_r.at[unit(n)], to_peer)

    def wait_s(u):
        whole = rcv.at[pl.ds(*span(u))]
        remote(whole, whole, 3, s_r.at[u], to_peer).wait_recv()

    def copy_zc(u, place):
        part = zall.at[pl.ds(*span(u)), place]
        return remote(part, part, 2, zn_r.at[max(0, u - EARLY_SPANS + 1)], to_near)

    def copy_zf(u, place):
        part = zall.at[pl.ds(*span(u)), place]
        return remote(part, part, 2, zn_r.at[max(0, u - EARLY_SPANS + 1)], to_near)

    def wait_zn(u):
        start, size = SPANS[u] if u >= EARLY_SPANS else (0, NJ)
        whole = zall.at[pl.ds(start, size), pl.ds(0, 2)]
        remote(whole, whole, 2, zn_r.at[max(0, u - EARLY_SPANS + 1)], to_near).wait_recv()

    def copy_zx(u, src, dst):
        ns = pl.ds(*span(u))
        return remote(zall.at[ns, src], zall.at[ns, dst], 2, zx_r.at[u], to_far)

    def out_cols(half, j):
        return out.at[:, pl.ds(pl.multiple_of(half * HALF + j * NC, NC), NC)]

    def copy_res(j, half):
        return remote(res.at[j], out_cols(half, j), 3, res_r.at[0], to_peer)

    barrier = pltpu.get_barrier_semaphore()
    for where in (to_near, to_far, to_diag, to_peer):
        pl.semaphore_signal(barrier, inc=1, device_id=where, device_id_type=MESH)
    load_lt = pltpu.make_async_copy(lt, ltall.at[core], local_sem.at[2])
    load_lt.start()
    for k in range(DIM // UNIT):
        load_tok(k).start()
    mine_x = xall.at[:, rows(core)]
    load_lt.wait()
    early, late = (xall.at[pl.ds(a, n), rows(core)] for a, n in ((0, EARLY_UNITS), (EARLY_UNITS, DIM // UNIT - EARLY_UNITS)))
    pltpu.make_async_copy(early, early, local_sem.at[0]).wait()
    with scope("barrier"):
        pl.semaphore_wait(barrier, 4)

    def send_pieces(ks):
        @pl.when(lead)
        def _():
            for k in ks:
                copy_b(k).start()
        for k in ks:
            copy_a(k, core).start()

    send_pieces(range(1))
    copy_lt(to_near, core).start()
    copy_lt(to_far, there).start()
    copy_lt(to_diag, there).start()
    send_pieces(range(1, EARLY))
    pltpu.make_async_copy(late, late, local_sem.at[1]).wait()
    send_pieces(range(EARLY, NP))
    for g, e in ((0, 0), (1, 0), (0, 1), (2, 0), (3, 0), (1, 1), (2, 1), (3, 1)):
        load_win(e, g).start()

    def relay_b(*ks):
        for k in ks:
            with scope(f"relayb{k}"):
                @pl.when(lead)
                def _():
                    copy_b(k).wait_recv()
                    copy_c(k).start()
                    if k < TWO_WAY:
                        copy_d(k, tp).start()

    def relay_d(*ks):
        for k in ks:
            with scope(f"relayd{k}"):
                @pl.when(lead)
                def _():
                    copy_d(k, peer).wait_recv()
                    copy_e(k).start()

    scores = ltall[core]
    grown = jnp.exp(scores - jnp.max(scores, axis=0, keepdims=True))
    probs[...] = grown / jnp.sum(grown, axis=0, keepdims=True)

    relay_b(0, 1)
    with scope("ltwait"):
        three = ltall.at[pl.ds(0, 3)]
        remote(three, three, 0, lt_r.at[0], to_near).wait_recv()

    below = jnp.where(lax.broadcasted_iota(jnp.int32, (128, 128), 0) < lax.broadcasted_iota(jnp.int32, (128, 128), 1),
                      1.0, 0.0).astype(BF16)
    before = jnp.where(lax.broadcasted_iota(jnp.int32, (8, 8), 1) < lax.broadcasted_iota(jnp.int32, (8, 8), 0),
                       1.0, 0.0).astype(BF16)

    first_half = lax.broadcasted_iota(jnp.int32, (HC, TOK), 0).astype(F32)

    def pick(i):
        expert = ep * OWN + i
        line = jnp.concatenate([ltall[p, pl.ds(expert, 1), :] for p in range(EP)], axis=1)
        rank = jnp.zeros((1, TOK), F32)
        for s in range(TOK // 128):
            wide = jnp.concatenate([column(line[:, s * 128:(s + 1) * 128])] * (TOK // 128), axis=1)
            rank = rank + jnp.sum(jnp.where(wide > line, 1.0, 0.0), axis=0, keepdims=True)
        taken = jnp.where(rank < CAP, 1.0, 0.0)
        grid = jnp.concatenate([taken[:, s * 128:(s + 1) * 128] for s in range(8)], axis=0)
        grid16 = grid.astype(BF16)
        inside = jnp.dot(grid16, below, preferred_element_type=F32)
        ahead = jnp.sum(jnp.dot(before, grid16, preferred_element_type=F32), axis=1, keepdims=True)
        slot = jnp.where(grid > 0.5, inside + ahead, -1.0)
        slots[core, i * 8:(i + 1) * 8, :] = slot
        slot = jnp.concatenate([slot[s:s + 1, :] for s in range(8)], axis=1)
        hot1[i * HC:(i + 1) * HC, :] = jnp.where(first_half[:, :3 * BLK] == slot[:, :3 * BLK], 1.0, 0.0).astype(BF16)

    def pick_late():
        for i in range(OWN):
            slot = jnp.concatenate([slots[core, i * 8 + s:i * 8 + s + 1, :] for s in range(8)], axis=1)
            hot2[i * HC:(i + 1) * HC, :] = jnp.where(first_half + HC == slot, 1.0, 0.0).astype(BF16)

    def cut(first_unit, units, place, places):
        part = pl.ds(place * BLK, places * BLK)
        return jnp.concatenate([xall[u, part, :] for u in range(first_unit, first_unit + units)], axis=1)

    def lanes_of(first_unit, units):
        return slice(first_unit * UNIT, (first_unit + units) * UNIT)

    def take_own(pairs):
        for u in pairs:
            xg[:, lanes_of(2 * u, 2)] = jnp.dot(hot1[:, :2 * BLK], cut(2 * u, 2, 0, 2), preferred_element_type=F32).astype(BF16)

    def take_a(units):
        for u, n in units:
            cols = lanes_of(u, n)
            r = jnp.dot(hot1[:, 2 * BLK:], cut(u, n, A, 1), preferred_element_type=F32)
            xg[:, cols] = (xg[:, cols].astype(F32) + r).astype(BF16)

    def first_tiles(h, e, first_unit, units, x):
        for n in range(HID // TILE):
            cols = slice(n * TILE, (n + 1) * TILE)
            r = jnp.dot(x, win[e, first_unit * UNIT:(first_unit + units) * UNIT, cols], preferred_element_type=F32)
            if first_unit > 0:
                r = r + acc[e, :, cols]
            if first_unit + units < DIM // UNIT:
                acc[e, :, cols] = r
            else:
                hid[h, e, :, cols] = gelu(r).astype(BF16)

    def first(e, first_unit, units):
        with scope(f"first{first_unit}e{e}"):
            for g in range(NG):
                if first_unit <= g * UG < first_unit + units:
                    wait_win(e, g)
            if e == 0:
                take_a([(u, 2) for u in range(first_unit, first_unit + units, 2)])
            first_tiles(0, e, first_unit, units, xg[e * HC:(e + 1) * HC, lanes_of(first_unit, units)])

    def first_late(g):
        for m in range(0, UG, 2):
            x = cut(UG * g + m, 2, 0, EP)
            xg2[:, m * UNIT:(m + 2) * UNIT] = jnp.dot(hot2[...], x, preferred_element_type=F32).astype(BF16)

        def body(e, _):
            first_tiles(1, e, UG * g, UG, xg2[pl.ds(pl.multiple_of(e * HC, HC), HC), :])
            return 0
        lax.fori_loop(0, OWN, body, 0)

    def second(m):
        h, j, e = order[m]
        n = h * NJ + j
        with scope(f"second{n}e{e}"):
            if m > 0:
                wait_wout(m)
            mid = slice(e * HC, (e + 1) * HC)
            r = jnp.dot(hid[h, e], wout[m % NB], preferred_element_type=F32)
            snd[n, mid, :] = r[:, :NC]
            mine[n, mid, :] = r[:, NC:]
            copy_s(n, e).start()
            load_wout(m + NB)

    def ready(*ks):
        with scope(f"ready{ks[0]}"):
            @pl.when(follow)
            def _():
                for k in ks:
                    copy_c(k).wait_recv()
                    if k == NP - 1:
                        for g in range(NG):
                            copy_g(g).start()
                    if k < TWO_WAY:
                        copy_e(k).wait_recv()

    relay_b(2)
    with scope("pick0"):
        pick(0)
    relay_b(3)
    with scope("pick1"):
        pick(1)
    relay_b(4)
    with scope("wait_a"):
        near_x = xall.at[:, rows(place_near)]
        remote(near_x, near_x, 1, a_r.at[0], to_near).wait_recv()
    relay_d(0, 1)
    with scope("own0"):
        take_own(range(4))
    relay_b(5)
    with scope("own1"):
        take_own(range(4, 8))
    relay_d(2)
    relay_b(6)
    ready(0, 1, 2)
    first(0, 0, 4)
    for m in range(NB):
        load_wout(m)
    relay_b(7)
    relay_d(3, 4)
    ready(3, 4)
    first(0, 4, 4)
    relay_d(5)
    relay_b(8)
    ready(5)
    first(0, 8, 2)
    ready(8)
    first(0, 12, 2)
    relay_d(6)
    relay_b(9)
    ready(6)
    first(0, 10, 2)
    wait_wout(0)
    relay_d(7)
    ready(7, 9)
    first(0, 14, 2)
    for m in range(len(head)):
        second(m)
    first(1, 0, 4)
    first(1, 4, 4)
    first(1, 8, 4)
    first(1, 12, 4)
    copy_slots(to_near, core).start()
    copy_slots(to_far, there).start()
    copy_slots(to_diag, there).start()

    def relay_g(g):
        with scope(f"relayg{g}"):
            @pl.when(follow)
            def _():
                copy_g(g).wait_recv()
                copy_f(g).start()

    half = OWN * NJ
    for m in range(len(head), half):
        second(m)
        if m in (half - 8, half - 2):
            relay_g(0 if m == half - 8 else 1)
    with scope("pick_late"):
        pick_late()
    for g in range(NG):
        if g > 0 and g + 1 < NG:
            relay_g(g + 1)
        with scope(f"readyB{g}"):
            @pl.when(lead)
            def _():
                copy_f(g).wait_recv()
        with scope(f"firstB{g}"):
            first_late(g)
    def close(u):
        with scope(f"waits{u}"):
            wait_s(u)
        start, size = span(u)
        for n in range(start, start + size):
            zall[n, core] = (mine[n] + rcv[n]).astype(BF16)
        copy_zx(u, core, there).start()
        copy_zc(u, core).start()

    def forward(u):
        with scope(f"waitzx{u}"):
            copy_zx(u, place_far, place_far).wait_recv()
        copy_zf(u, place_far).start()

    def combine(j):
        total = jnp.zeros((BLK, NC), F32)
        for p in range(EP):
            for i in range(OWN):
                mid = slice(i * HC, (i + 1) * HC)
                z = jnp.concatenate([zall[j, p, mid, :], zall[NJ + j, p, mid, :]], axis=0)
                total = total + gate[p * OWN + i] * jnp.dot(back[p * OWN + i], z, preferred_element_type=F32)
        own = xall[tp * NJ + j, rows(core), :]
        res[j] = (own.astype(F32) + total).astype(BF16)
        copy_res(j, tp).start()
        out[:, pl.ds(pl.multiple_of(tp * HALF + j * NC, NC), NC)] = res[j]

    close(0)
    for m in range(half, 2 * half):
        second(m)


    with scope("slotwait"):
        three = slots.at[pl.ds(0, 3)]
        remote(three, three, 0, sl_r.at[0], to_near).wait_recv()
    with scope("back"):
        lanes = lax.broadcasted_iota(jnp.int32, (128, CAP), 1).astype(F32)
        for p in range(EP):
            mark = core if p < 2 else there
            owner = 2 * chip + p if p < 2 else 2 * (1 - chip) + (3 - p)
            for i in range(OWN):
                for c in range(BLK // 128):
                    part = slice(c * 128, (c + 1) * 128)
                    col = column(slots[p, pl.ds(i * 8 + mark * 2 + c, 1), :])
                    back[p * OWN + i, part, :] = jnp.where(jnp.concatenate([col, col], axis=1) == lanes, 1.0, 0.0).astype(BF16)
                    gate[p * OWN + i, part, :] = column(probs[pl.ds(owner * OWN + i, 1), :][:, part])

    units = len(SPANS)
    for u in range(1, units + 2):
        if u < units:
            close(u)
        if u - 1 < units:
            forward(u - 1)
        if u - 2 >= EARLY_SPANS:
            with scope(f"waitzn{u - 2}"):
                if u - 2 == EARLY_SPANS:
                    wait_zn(0)
                wait_zn(u - 2)
            start, size = span(u - 2)
            for n in range(start, start + size):
                combine(n - NJ)

    with scope("drain"):
        def left(ref, family):
            remote(ref, ref, family, res_r.at[0], to_near).wait_send()
        left(rcv.at[0, pl.ds(0, 96)], 0)
        left(zall.at[pl.ds(0, 12)], 1)
        left(zall.at[pl.ds(0, 12)], 2)
        left(zall.at[pl.ds(0, 10)], 3)
        remote(res, res, 3, res_r.at[0], to_peer).wait_recv()


def solution(mesh):
    def local_layer(tokens, logits, w_in, w_out):
        dma = pltpu.SemaphoreType.DMA
        units = len(SPANS)
        scratch = [
            pltpu.VMEM((DIM // UNIT, TOK, UNIT), BF16),
            pltpu.VMEM((EP, EXPERTS, BLK), F32),
            pltpu.VMEM((EP, OWN * 8, 128), F32),
            pltpu.VMEM((OWN * HC, 3 * BLK), BF16),
            pltpu.VMEM((OWN * HC, TOK), BF16),
            pltpu.VMEM((OWN * HC, DIM), BF16),
            pltpu.VMEM((OWN * HC, KG), BF16),
            pltpu.VMEM((OWN, DIM, HID), BF16),
            pltpu.VMEM((OWN, HC, HID), F32),
            pltpu.VMEM((2, OWN, HC, HID), BF16),
            pltpu.VMEM((NB, HID, 2 * NC), BF16),
            pltpu.VMEM((2 * NJ, OWN * HC, NC), F32),
            pltpu.VMEM((2 * NJ, OWN * HC, NC), F32),
            pltpu.VMEM((2 * NJ, OWN * HC, NC), F32),
            pltpu.VMEM((2 * NJ, EP, OWN * HC, NC), BF16),
            pltpu.VMEM((EXPERTS, BLK, CAP), BF16),
            pltpu.VMEM((EXPERTS, BLK, NC), F32),
            pltpu.VMEM((EXPERTS, BLK), F32),
            pltpu.VMEM((NJ, BLK, NC), BF16),
            dma((3,)), dma((OWN * NG,)), dma((NB,)), dma((4,)),
            dma((1,)), dma((1,)), dma((1,)), dma((NP,)), dma((TWO_WAY,)), dma((NG,)),
            dma((units,)), dma((units,)), dma((1 + units - EARLY_SPANS,)), dma((1,)),
        ]
        return pl.pallas_call(
            kernel,
            out_shape=pltpu.VMEM(tokens.shape, BF16),
            in_specs=[pl.BlockSpec(memory_space=pl.ANY), pl.BlockSpec(memory_space=pl.ANY),
                      pl.BlockSpec(memory_space=pl.ANY), pl.BlockSpec(memory_space=pl.ANY)],
            out_specs=pl.BlockSpec(memory_space=pltpu.VMEM),
            scratch_shapes=scratch,
            compiler_params=pltpu.CompilerParams(collective_id=0, has_side_effects=True,
                                                 vmem_limit_bytes=62_500_000),
            name="moe_layer",
        )(tokens, logits.T, w_in, w_out)

    row_spec = P(("dp", "ep"), None)
    return jax.shard_map(local_layer, mesh=mesh,
                         in_specs=(row_spec, row_spec, P("ep", None, "tp"), P("ep", "tp", None)),
                         out_specs=row_spec, check_vma=False)
```

```python
import jax
import jax.numpy as jnp
from jax import lax
from jax.experimental import pallas as pl
from jax.experimental.pallas import tpu as pltpu
from jax.sharding import PartitionSpec as P

MESH = pl.DeviceIdType.MESH
F32 = jnp.float32
BF16 = jnp.bfloat16

BLK = 256
XR = 128
YR = BLK - XR
EXPERTS = 8
OWN = 2
CAP = 256
HC = CAP // 2
DIM = 2048
HID = 2816
EP = 4
TOK = BLK * EP
HALF = DIM // 2
UNIT = 128
PIECES = [(0, 1), (1, 1), (2, 2), (4, 2), (6, 2), (8, 2), (12, 2), (14, 1), (10, 2), (15, 1)]
TWO_WAY = 8
NP = len(PIECES)
NG = 4
KG = DIM // NG
UG = KG // UNIT
NJ = 8
NC = HALF // NJ
SPANS = [(0, 4), (4, 4), (8, 2), (10, 2), (12, 2), (14, 1), (15, 1)]
EARLY_SPANS = 2
NB = 6
TILE = 256
EARLY = 3
EARLY_UNITS = 4


def gelu(v):
    return 0.5 * v * (1.0 + jnp.tanh(v * (0.7978845608028654 + 0.035677408136300125 * (v * v))))


def column(row):
    return jnp.transpose(jnp.broadcast_to(row, (128, 128)))


def kernel(tok, lt, w_in, w_out, out,
           xall, ltall, slots, hot1, hot2, xg, xg2, win, acc, hid, wout, snd, mine, rcv, zall, back, gate, probs, res,
           local_sem, win_sem, wout_sem, send, lt_r, sl_r, a_r, bc_r, de_r, gf_r, s_r, zx_r, zn_r, res_r):
    scope = jax.named_scope
    ep = lax.axis_index("ep")
    tp = lax.axis_index("tp")
    core = lax.rem(ep, 2)
    chip = ep // 2
    near = ep + 1 - 2 * core
    far = lax.rem(ep + 2, 4)
    diag = 3 - ep
    peer = 1 - tp
    to_near, to_far, to_diag = {"ep": near, "tp": tp}, {"ep": far, "tp": tp}, {"ep": diag, "tp": tp}
    to_peer = {"ep": ep, "tp": peer}
    A, B = 2, 3
    place_near, place_far, place_diag = 1 - core, 3 - core, 2 + core
    there = 3 - core
    lead, follow = core == 1, core == 0

    def rows(place, offset=0, size=BLK):
        return pl.ds(pl.multiple_of(place * BLK + offset, 32), size)

    def remote(src, dst, family, recv, where):
        return pltpu.make_async_remote_copy(src_ref=src, dst_ref=dst, send_sem=send.at[family], recv_sem=recv,
                                            device_id=where, device_id_type=MESH)

    def load_tok(k):
        return pltpu.make_async_copy(tok.at[:, pl.ds(k * UNIT, UNIT)], xall.at[k, rows(core)], local_sem.at[0 if k < EARLY_UNITS else 1])

    def load_win(e, g):
        part = pl.ds(g * KG, KG)
        return pltpu.make_async_copy(w_in.at[e, part], win.at[e, part], win_sem.at[g if e == 0 else NG])

    def wait_win(e, g):
        if e == 0:
            load_win(e, g).wait()
        elif g == 0:
            pltpu.make_async_copy(win.at[e], win.at[e], win_sem.at[NG]).wait()

    head = [(0, 0, 0), (0, 1, 0), (0, 2, 0)]
    order = head + [(0, 3, 0)] + [(0, j, 1) for j in range(4)]
    order += [(0, j, e) for j in range(4, NJ) for e in range(OWN)] + [(1, j, e) for j in range(NJ) for e in range(OWN)]

    def load_wout(m):
        if m >= len(order):
            return
        _, j, e = order[m]
        for side, half in enumerate((peer, tp)):
            cols = pl.ds(pl.multiple_of(half * HALF + j * NC, NC), NC)
            pltpu.make_async_copy(w_out.at[e, :, cols], wout.at[m % NB, :, pl.ds(side * NC, NC)], wout_sem.at[m % NB]).start()

    def wait_wout(m):
        both = wout.at[m % NB]
        pltpu.make_async_copy(both, both, wout_sem.at[m % NB]).wait()

    def copy_lt(where, place):
        return remote(ltall.at[core], ltall.at[place], 0, lt_r.at[0], where)

    def copy_slots(where, place):
        return remote(slots.at[core], slots.at[place], 0, sl_r.at[0], where)

    def copy_a(k, place):
        piece = xall.at[pl.ds(*PIECES[k]), rows(place)]
        return remote(piece, piece, 1, a_r.at[0], to_near)

    def b_rows(k, place):
        return rows(place, tp * YR, XR) if k < TWO_WAY else rows(place)

    def copy_b(k):
        units = pl.ds(*PIECES[k])
        return remote(xall.at[units, b_rows(k, core)], xall.at[units, b_rows(k, A)], 1, bc_r.at[k], to_far)

    def copy_c(k):
        piece = xall.at[pl.ds(*PIECES[k]), b_rows(k, A)]
        return remote(piece, piece, 1, bc_r.at[k], to_near)

    def copy_d(k, half):
        piece = xall.at[pl.ds(*PIECES[k]), rows(A, half * XR, YR)]
        return remote(piece, piece, 1, de_r.at[k], to_peer)

    def copy_e(k):
        piece = xall.at[pl.ds(*PIECES[k]), rows(A, peer * XR, YR)]
        return remote(piece, piece, 1, de_r.at[k], to_near)

    def copy_g(g):
        group = pl.ds(UG * g, UG)
        return remote(xall.at[group, rows(core)], xall.at[group, rows(B)], 1, gf_r.at[g], to_far)

    def copy_f(g):
        group = xall.at[pl.ds(UG * g, UG), rows(B)]
        return remote(group, group, 1, gf_r.at[g], to_near)

    def span(u):
        return SPANS[u]

    def unit(n):
        return [u for u, (start, size) in enumerate(SPANS) if start <= n < start + size][0]

    def copy_s(n, e):
        mid = pl.ds(e * HC, HC)
        return remote(snd.at[n, mid], rcv.at[n, mid], 3, s_r.at[unit(n)], to_peer)

    def wait_s(u):
        whole = rcv.at[pl.ds(*span(u))]
        remote(whole, whole, 3, s_r.at[u], to_peer).wait_recv()

    def copy_zc(u, place):
        part = zall.at[pl.ds(*span(u)), place]
        return remote(part, part, 2, zn_r.at[max(0, u - EARLY_SPANS + 1)], to_near)

    def copy_zf(u, place):
        part = zall.at[pl.ds(*span(u)), place]
        return remote(part, part, 2, zn_r.at[max(0, u - EARLY_SPANS + 1)], to_near)

    def wait_zn(u):
        start, size = SPANS[u] if u >= EARLY_SPANS else (0, NJ)
        whole = zall.at[pl.ds(start, size), pl.ds(0, 2)]
        remote(whole, whole, 2, zn_r.at[max(0, u - EARLY_SPANS + 1)], to_near).wait_recv()

    def copy_zx(u, src, dst):
        ns = pl.ds(*span(u))
        return remote(zall.at[ns, src], zall.at[ns, dst], 2, zx_r.at[u], to_far)

    def out_cols(half, j):
        return out.at[:, pl.ds(pl.multiple_of(half * HALF + j * NC, NC), NC)]

    def copy_res(j, half):
        return remote(res.at[j], out_cols(half, j), 3, res_r.at[0], to_peer)

    barrier = pltpu.get_barrier_semaphore()
    for where in (to_near, to_far, to_diag, to_peer):
        pl.semaphore_signal(barrier, inc=1, device_id=where, device_id_type=MESH)
    load_lt = pltpu.make_async_copy(lt, ltall.at[core], local_sem.at[2])
    load_lt.start()
    for k in range(DIM // UNIT):
        load_tok(k).start()
    mine_x = xall.at[:, rows(core)]
    load_lt.wait()
    early, late = (xall.at[pl.ds(a, n), rows(core)] for a, n in ((0, EARLY_UNITS), (EARLY_UNITS, DIM // UNIT - EARLY_UNITS)))
    pltpu.make_async_copy(early, early, local_sem.at[0]).wait()
    with scope("barrier"):
        pl.semaphore_wait(barrier, 4)

    def send_pieces(ks):
        @pl.when(lead)
        def _():
            for k in ks:
                copy_b(k).start()
        for k in ks:
            copy_a(k, core).start()

    send_pieces(range(1))
    copy_lt(to_near, core).start()
    copy_lt(to_far, there).start()
    copy_lt(to_diag, there).start()
    send_pieces(range(1, EARLY))
    pltpu.make_async_copy(late, late, local_sem.at[1]).wait()
    send_pieces(range(EARLY, NP))
    for g, e in ((0, 0), (1, 0), (0, 1), (2, 0), (3, 0), (1, 1), (2, 1), (3, 1)):
        load_win(e, g).start()

    def relay_b(*ks):
        for k in ks:
            with scope(f"relayb{k}"):
                @pl.when(lead)
                def _():
                    copy_b(k).wait_recv()
                    copy_c(k).start()
                    if k < TWO_WAY:
                        copy_d(k, tp).start()

    def relay_d(*ks):
        for k in ks:
            with scope(f"relayd{k}"):
                @pl.when(lead)
                def _():
                    copy_d(k, peer).wait_recv()
                    copy_e(k).start()

    scores = ltall[core]
    grown = jnp.exp(scores - jnp.max(scores, axis=0, keepdims=True))
    probs[...] = grown / jnp.sum(grown, axis=0, keepdims=True)

    relay_b(0, 1)
    with scope("ltwait"):
        three = ltall.at[pl.ds(0, 3)]
        remote(three, three, 0, lt_r.at[0], to_near).wait_recv()

    below = jnp.where(lax.broadcasted_iota(jnp.int32, (128, 128), 0) < lax.broadcasted_iota(jnp.int32, (128, 128), 1),
                      1.0, 0.0).astype(BF16)
    before = jnp.where(lax.broadcasted_iota(jnp.int32, (8, 8), 1) < lax.broadcasted_iota(jnp.int32, (8, 8), 0),
                       1.0, 0.0).astype(BF16)

    first_half = lax.broadcasted_iota(jnp.int32, (HC, TOK), 0).astype(F32)

    def pick(i):
        expert = ep * OWN + i
        line = jnp.concatenate([ltall[p, pl.ds(expert, 1), :] for p in range(EP)], axis=1)
        rank = jnp.zeros((1, TOK), F32)
        for s in range(TOK // 128):
            wide = jnp.concatenate([column(line[:, s * 128:(s + 1) * 128])] * (TOK // 128), axis=1)
            rank = rank + jnp.sum(jnp.where(wide > line, 1.0, 0.0), axis=0, keepdims=True)
        taken = jnp.where(rank < CAP, 1.0, 0.0)
        grid = jnp.concatenate([taken[:, s * 128:(s + 1) * 128] for s in range(8)], axis=0)
        grid16 = grid.astype(BF16)
        inside = jnp.dot(grid16, below, preferred_element_type=F32)
        ahead = jnp.sum(jnp.dot(before, grid16, preferred_element_type=F32), axis=1, keepdims=True)
        slot = jnp.where(grid > 0.5, inside + ahead, -1.0)
        slots[core, i * 8:(i + 1) * 8, :] = slot
        slot = jnp.concatenate([slot[s:s + 1, :] for s in range(8)], axis=1)
        hot1[i * HC:(i + 1) * HC, :] = jnp.where(first_half[:, :3 * BLK] == slot[:, :3 * BLK], 1.0, 0.0).astype(BF16)

    def pick_late():
        for i in range(OWN):
            slot = jnp.concatenate([slots[core, i * 8 + s:i * 8 + s + 1, :] for s in range(8)], axis=1)
            hot2[i * HC:(i + 1) * HC, :] = jnp.where(first_half + HC == slot, 1.0, 0.0).astype(BF16)

    def cut(first_unit, units, place, places):
        part = pl.ds(place * BLK, places * BLK)
        return jnp.concatenate([xall[u, part, :] for u in range(first_unit, first_unit + units)], axis=1)

    def lanes_of(first_unit, units):
        return slice(first_unit * UNIT, (first_unit + units) * UNIT)

    def take_own(pairs):
        for u in pairs:
            xg[:, lanes_of(2 * u, 2)] = jnp.dot(hot1[:, :2 * BLK], cut(2 * u, 2, 0, 2), preferred_element_type=F32).astype(BF16)

    def take_a(e, units):
        mid = slice(e * HC, (e + 1) * HC)
        for u, n in units:
            cols = lanes_of(u, n)
            r = jnp.dot(hot1[mid, 2 * BLK:], cut(u, n, A, 1), preferred_element_type=F32)
            xg[mid, cols] = (xg[mid, cols].astype(F32) + r).astype(BF16)

    def first_tiles(h, e, first_unit, units, x, w_next=None):
        z = None
        for n in range(HID // TILE):
            cols = slice(n * TILE, (n + 1) * TILE)
            r = jnp.dot(x, win[e, first_unit * UNIT:(first_unit + units) * UNIT, cols], preferred_element_type=F32)
            if first_unit > 0:
                r = r + acc[e, :, cols]
            if first_unit + units < DIM // UNIT:
                acc[e, :, cols] = r
            else:
                part = gelu(r).astype(BF16)
                hid[h, e, :, cols] = part
                if w_next is not None:
                    step = jnp.dot(part, w_next[cols, :], preferred_element_type=F32)
                    z = step if z is None else z + step
        return z

    def first(e, first_unit, units, w_next=None):
        with scope(f"first{first_unit}e{e}"):
            for g in range(NG):
                if first_unit <= g * UG < first_unit + units:
                    wait_win(e, g)
            take_a(e, [(u, 2) for u in range(first_unit, first_unit + units, 2)])
            return first_tiles(0, e, first_unit, units, xg[e * HC:(e + 1) * HC, lanes_of(first_unit, units)], w_next)

    def first_late(g):
        for m in range(0, UG, 2):
            x = cut(UG * g + m, 2, 0, EP)
            xg2[:, m * UNIT:(m + 2) * UNIT] = jnp.dot(hot2[...], x, preferred_element_type=F32).astype(BF16)

        def body(e, _):
            first_tiles(1, e, UG * g, UG, xg2[pl.ds(pl.multiple_of(e * HC, HC), HC), :])
            return 0
        lax.fori_loop(0, OWN, body, 0)

    def second(m, r=None):
        h, j, e = order[m]
        n = h * NJ + j
        with scope(f"second{n}e{e}"):
            if m > 0:
                wait_wout(m)
            mid = slice(e * HC, (e + 1) * HC)
            if r is None:
                r = jnp.dot(hid[h, e], wout[m % NB], preferred_element_type=F32)
            snd[n, mid, :] = r[:, :NC]
            mine[n, mid, :] = r[:, NC:]
            copy_s(n, e).start()
            load_wout(m + NB)

    def ready(*ks):
        with scope(f"ready{ks[0]}"):
            @pl.when(follow)
            def _():
                for k in ks:
                    copy_c(k).wait_recv()
                    if k == NP - 1:
                        for g in range(NG):
                            copy_g(g).start()
                    if k < TWO_WAY:
                        copy_e(k).wait_recv()

    relay_b(2)
    with scope("pick0"):
        pick(0)
    relay_b(3)
    with scope("pick1"):
        pick(1)
    relay_b(4)
    with scope("wait_a"):
        near_x = xall.at[:, rows(place_near)]
        remote(near_x, near_x, 1, a_r.at[0], to_near).wait_recv()
    relay_d(0, 1)
    with scope("own0"):
        take_own(range(4))
    relay_b(5)
    with scope("own1"):
        take_own(range(4, 8))
    relay_d(2)
    relay_b(6)
    ready(0, 1, 2)
    first(0, 0, 4)
    for m in range(NB):
        load_wout(m)
    relay_b(7)
    relay_d(3, 4)
    ready(3, 4)
    first(0, 4, 4)
    relay_d(5)
    ready(5)
    first(0, 8, 2)
    relay_b(8)
    ready(8)
    first(0, 10, 2)
    relay_d(6)
    relay_b(9)
    ready(6)
    first(0, 12, 2)
    wait_wout(0)
    relay_d(7)
    ready(7, 9)
    second(0, first(0, 14, 2, wout.at[0]))
    for m in range(1, len(head)):
        second(m)
    first(1, 0, 4)
    first(1, 4, 4)
    first(1, 8, 4)
    first(1, 12, 4)
    copy_slots(to_near, core).start()
    copy_slots(to_far, there).start()
    copy_slots(to_diag, there).start()

    def relay_g(g):
        with scope(f"relayg{g}"):
            @pl.when(follow)
            def _():
                copy_g(g).wait_recv()
                copy_f(g).start()

    half = OWN * NJ
    for m in range(len(head), half):
        second(m)
        if m in (half - 8, half - 2):
            relay_g(0 if m == half - 8 else 1)
    with scope("pick_late"):
        pick_late()
    for g in range(NG):
        if g > 0 and g + 1 < NG:
            relay_g(g + 1)
        with scope(f"readyB{g}"):
            @pl.when(lead)
            def _():
                copy_f(g).wait_recv()
        with scope(f"firstB{g}"):
            first_late(g)
    def close(u):
        with scope(f"waits{u}"):
            wait_s(u)
        start, size = span(u)
        for n in range(start, start + size):
            zall[n, core] = (mine[n] + rcv[n]).astype(BF16)
        copy_zx(u, core, there).start()
        copy_zc(u, core).start()

    def forward(u):
        with scope(f"waitzx{u}"):
            copy_zx(u, place_far, place_far).wait_recv()
        copy_zf(u, place_far).start()

    def combine(j):
        total = jnp.zeros((BLK, NC), F32)
        for p in range(EP):
            for i in range(OWN):
                mid = slice(i * HC, (i + 1) * HC)
                z = jnp.concatenate([zall[j, p, mid, :], zall[NJ + j, p, mid, :]], axis=0)
                total = total + gate[p * OWN + i] * jnp.dot(back[p * OWN + i], z, preferred_element_type=F32)
        own = xall[tp * NJ + j, rows(core), :]
        res[j] = (own.astype(F32) + total).astype(BF16)
        copy_res(j, tp).start()
        out[:, pl.ds(pl.multiple_of(tp * HALF + j * NC, NC), NC)] = res[j]

    close(0)
    for m in range(half, 2 * half):
        second(m)


    with scope("slotwait"):
        three = slots.at[pl.ds(0, 3)]
        remote(three, three, 0, sl_r.at[0], to_near).wait_recv()
    with scope("back"):
        lanes = lax.broadcasted_iota(jnp.int32, (128, CAP), 1).astype(F32)
        for p in range(EP):
            mark = core if p < 2 else there
            owner = 2 * chip + p if p < 2 else 2 * (1 - chip) + (3 - p)
            for i in range(OWN):
                for c in range(BLK // 128):
                    part = slice(c * 128, (c + 1) * 128)
                    col = column(slots[p, pl.ds(i * 8 + mark * 2 + c, 1), :])
                    back[p * OWN + i, part, :] = jnp.where(jnp.concatenate([col, col], axis=1) == lanes, 1.0, 0.0).astype(BF16)
                    gate[p * OWN + i, part, :] = column(probs[pl.ds(owner * OWN + i, 1), :][:, part])

    units = len(SPANS)
    for u in range(1, units + 2):
        if u < units:
            close(u)
        if u - 1 < units:
            forward(u - 1)
        if u - 2 >= EARLY_SPANS:
            with scope(f"waitzn{u - 2}"):
                if u - 2 == EARLY_SPANS:
                    wait_zn(0)
                wait_zn(u - 2)
            start, size = span(u - 2)
            for n in range(start, start + size):
                combine(n - NJ)

    with scope("drain"):
        def left(ref, family):
            remote(ref, ref, family, res_r.at[0], to_near).wait_send()
        left(rcv.at[0, pl.ds(0, 96)], 0)
        left(zall.at[pl.ds(0, 12)], 1)
        left(zall.at[pl.ds(0, 12)], 2)
        left(zall.at[pl.ds(0, 10)], 3)
        remote(res, res, 3, res_r.at[0], to_peer).wait_recv()


def solution(mesh):
    def local_layer(tokens, logits, w_in, w_out):
        dma = pltpu.SemaphoreType.DMA
        units = len(SPANS)
        scratch = [
            pltpu.VMEM((DIM // UNIT, TOK, UNIT), BF16),
            pltpu.VMEM((EP, EXPERTS, BLK), F32),
            pltpu.VMEM((EP, OWN * 8, 128), F32),
            pltpu.VMEM((OWN * HC, 3 * BLK), BF16),
            pltpu.VMEM((OWN * HC, TOK), BF16),
            pltpu.VMEM((OWN * HC, DIM), BF16),
            pltpu.VMEM((OWN * HC, KG), BF16),
            pltpu.VMEM((OWN, DIM, HID), BF16),
            pltpu.VMEM((OWN, HC, HID), F32),
            pltpu.VMEM((2, OWN, HC, HID), BF16),
            pltpu.VMEM((NB, HID, 2 * NC), BF16),
            pltpu.VMEM((2 * NJ, OWN * HC, NC), F32),
            pltpu.VMEM((2 * NJ, OWN * HC, NC), F32),
            pltpu.VMEM((2 * NJ, OWN * HC, NC), F32),
            pltpu.VMEM((2 * NJ, EP, OWN * HC, NC), BF16),
            pltpu.VMEM((EXPERTS, BLK, CAP), BF16),
            pltpu.VMEM((EXPERTS, BLK, NC), F32),
            pltpu.VMEM((EXPERTS, BLK), F32),
            pltpu.VMEM((NJ, BLK, NC), BF16),
            dma((3,)), dma((NG + 1,)), dma((NB,)), dma((4,)),
            dma((1,)), dma((1,)), dma((1,)), dma((NP,)), dma((TWO_WAY,)), dma((NG,)),
            dma((units,)), dma((units,)), dma((1 + units - EARLY_SPANS,)), dma((1,)),
        ]
        return pl.pallas_call(
            kernel,
            out_shape=pltpu.VMEM(tokens.shape, BF16),
            in_specs=[pl.BlockSpec(memory_space=pl.ANY), pl.BlockSpec(memory_space=pl.ANY),
                      pl.BlockSpec(memory_space=pl.ANY), pl.BlockSpec(memory_space=pl.ANY)],
            out_specs=pl.BlockSpec(memory_space=pltpu.VMEM),
            scratch_shapes=scratch,
            compiler_params=pltpu.CompilerParams(collective_id=0, has_side_effects=True,
                                                 vmem_limit_bytes=62_500_000),
            name="moe_layer",
        )(tokens, logits.T, w_in, w_out)

    row_spec = P(("dp", "ep"), None)
    return jax.shard_map(local_layer, mesh=mesh,
                         in_specs=(row_spec, row_spec, P("ep", None, "tp"), P("ep", "tp", None)),
                         out_specs=row_spec, check_vma=False)
```

```python
import jax
import jax.numpy as jnp
from jax import lax
from jax.experimental import pallas as pl
from jax.experimental.pallas import tpu as pltpu
from jax.sharding import PartitionSpec as P

MESH = pl.DeviceIdType.MESH
F32 = jnp.float32
BF16 = jnp.bfloat16

BLK = 256
XR = 128
YR = BLK - XR
EXPERTS = 8
OWN = 2
CAP = 256
HC = CAP // 2
DIM = 2048
HID = 2816
EP = 4
TOK = BLK * EP
HALF = DIM // 2
UNIT = 128
PIECES = [(0, 1), (1, 1), (2, 2), (4, 2), (6, 2), (8, 2), (12, 2), (14, 1), (10, 2), (15, 1)]
TWO_WAY = 8
NP = len(PIECES)
NG = 4
KG = DIM // NG
UG = KG // UNIT
NJ = 8
NC = HALF // NJ
SPANS = [(0, 4), (4, 4), (8, 2), (10, 2), (12, 2), (14, 1), (15, 1)]
EARLY_SPANS = 2
NB = 6
TILE = 256
EARLY = 3
EARLY_UNITS = 4


def gelu(v):
    return 0.5 * v * (1.0 + jnp.tanh(v * (0.7978845608028654 + 0.035677408136300125 * (v * v))))


def column(row):
    return jnp.transpose(jnp.broadcast_to(row, (128, 128)))


def kernel(tok, lt, w_in, w_out, out,
           xall, score, ltsend, ltall, slots, hot1, hot2, xg, xg2, win, acc, hid, wout, snd, mine, rcv, zall, back, gate, probs, res,
           local_sem, win_sem, wout_sem, send, lt_r, sl_r, a_r, bc_r, de_r, gf_r, s_r, zx_r, zn_r, res_r):
    scope = jax.named_scope
    ep = lax.axis_index("ep")
    tp = lax.axis_index("tp")
    core = lax.rem(ep, 2)
    chip = ep // 2
    near = ep + 1 - 2 * core
    far = lax.rem(ep + 2, 4)
    diag = 3 - ep
    peer = 1 - tp
    to_near, to_far, to_diag = {"ep": near, "tp": tp}, {"ep": far, "tp": tp}, {"ep": diag, "tp": tp}
    to_peer = {"ep": ep, "tp": peer}
    A, B = 2, 3
    place_near, place_far, place_diag = 1 - core, 3 - core, 2 + core
    there = 3 - core
    lead, follow = core == 1, core == 0

    def rows(place, offset=0, size=BLK):
        return pl.ds(pl.multiple_of(place * BLK + offset, 32), size)

    def remote(src, dst, family, recv, where):
        return pltpu.make_async_remote_copy(src_ref=src, dst_ref=dst, send_sem=send.at[family], recv_sem=recv,
                                            device_id=where, device_id_type=MESH)

    def load_tok(k):
        return pltpu.make_async_copy(tok.at[:, pl.ds(k * UNIT, UNIT)], xall.at[k, rows(core)], local_sem.at[0 if k < EARLY_UNITS else 1])

    def load_win(e, g):
        part = pl.ds(g * KG, KG)
        return pltpu.make_async_copy(w_in.at[e, part], win.at[e, part], win_sem.at[g if e == 0 else NG])

    def wait_win(e, g):
        if e == 0:
            load_win(e, g).wait()
        elif g == 0:
            pltpu.make_async_copy(win.at[e], win.at[e], win_sem.at[NG]).wait()

    head = [(0, j, 0) for j in range(4)]
    order = head + [(0, j, 1) for j in range(4)]
    order += [(0, j, e) for j in range(4, NJ) for e in range(OWN)] + [(1, j, e) for j in range(NJ) for e in range(OWN)]

    def load_wout(m):
        if m >= len(order):
            return
        _, j, e = order[m]
        for side, half in enumerate((peer, tp)):
            cols = pl.ds(pl.multiple_of(half * HALF + j * NC, NC), NC)
            pltpu.make_async_copy(w_out.at[e, :, cols], wout.at[m % NB, :, pl.ds(side * NC, NC)], wout_sem.at[m % NB]).start()

    def wait_wout(m):
        both = wout.at[m % NB]
        pltpu.make_async_copy(both, both, wout_sem.at[m % NB]).wait()

    def copy_lt(where, target, place):
        return remote(ltsend.at[target], ltall.at[place], 4, lt_r.at[0], where)

    def copy_slots(where, place):
        return remote(slots.at[core], slots.at[place], 0, sl_r.at[0], where)

    def copy_a(k, place):
        piece = xall.at[pl.ds(*PIECES[k]), rows(place)]
        return remote(piece, piece, 1, a_r.at[0], to_near)

    def b_rows(k, place):
        return rows(place, tp * YR, XR) if k < TWO_WAY else rows(place)

    def copy_b(k):
        units = pl.ds(*PIECES[k])
        return remote(xall.at[units, b_rows(k, core)], xall.at[units, b_rows(k, A)], 1, bc_r.at[k], to_far)

    def copy_c(k):
        piece = xall.at[pl.ds(*PIECES[k]), b_rows(k, A)]
        return remote(piece, piece, 1, bc_r.at[k], to_near)

    def copy_d(k, half):
        piece = xall.at[pl.ds(*PIECES[k]), rows(A, half * XR, YR)]
        return remote(piece, piece, 1, de_r.at[k], to_peer)

    def copy_e(k):
        piece = xall.at[pl.ds(*PIECES[k]), rows(A, peer * XR, YR)]
        return remote(piece, piece, 1, de_r.at[k], to_near)

    def copy_g(g):
        group = pl.ds(UG * g, UG)
        return remote(xall.at[group, rows(core)], xall.at[group, rows(B)], 1, gf_r.at[g], to_far)

    def copy_f(g):
        group = xall.at[pl.ds(UG * g, UG), rows(B)]
        return remote(group, group, 1, gf_r.at[g], to_near)

    def span(u):
        return SPANS[u]

    def unit(n):
        return [u for u, (start, size) in enumerate(SPANS) if start <= n < start + size][0]

    def copy_s(n, e):
        mid = pl.ds(e * HC, HC)
        return remote(snd.at[n, mid], rcv.at[n, mid], 3, s_r.at[unit(n)], to_peer)

    def wait_s(u):
        whole = rcv.at[pl.ds(*span(u))]
        remote(whole, whole, 3, s_r.at[u], to_peer).wait_recv()

    def copy_zc(u, place):
        part = zall.at[pl.ds(*span(u)), place]
        return remote(part, part, 2, zn_r.at[max(0, u - EARLY_SPANS + 1)], to_near)

    def copy_zf(u, place):
        part = zall.at[pl.ds(*span(u)), place]
        return remote(part, part, 2, zn_r.at[max(0, u - EARLY_SPANS + 1)], to_near)

    def wait_zn(u):
        start, size = SPANS[u] if u >= EARLY_SPANS else (0, NJ)
        whole = zall.at[pl.ds(start, size), pl.ds(0, 2)]
        remote(whole, whole, 2, zn_r.at[max(0, u - EARLY_SPANS + 1)], to_near).wait_recv()

    def copy_zx(u, src, dst):
        ns = pl.ds(*span(u))
        return remote(zall.at[ns, src], zall.at[ns, dst], 2, zx_r.at[u], to_far)

    def out_cols(half, j):
        return out.at[:, pl.ds(pl.multiple_of(half * HALF + j * NC, NC), NC)]

    def copy_res(j, half):
        return remote(res.at[j], out_cols(half, j), 3, res_r.at[0], to_peer)

    barrier = pltpu.get_barrier_semaphore()
    for where in (to_near, to_far, to_diag, to_peer):
        pl.semaphore_signal(barrier, inc=1, device_id=where, device_id_type=MESH)
    load_lt = pltpu.make_async_copy(lt, score, local_sem.at[2])
    load_lt.start()
    for k in range(DIM // UNIT):
        load_tok(k).start()
    mine_x = xall.at[:, rows(core)]
    load_lt.wait()
    for d in range(EP):
        ltsend[d] = score[d * OWN:(d + 1) * OWN, :]
    early, late = (xall.at[pl.ds(a, n), rows(core)] for a, n in ((0, EARLY_UNITS), (EARLY_UNITS, DIM // UNIT - EARLY_UNITS)))
    pltpu.make_async_copy(early, early, local_sem.at[0]).wait()
    with scope("barrier"):
        pl.semaphore_wait(barrier, 4)

    def send_pieces(ks):
        @pl.when(lead)
        def _():
            for k in ks:
                copy_b(k).start()
        for k in ks:
            copy_a(k, core).start()

    send_pieces(range(1))
    copy_lt(to_near, near, core).start()
    copy_lt(to_far, far, there).start()
    copy_lt(to_diag, diag, there).start()
    send_pieces(range(1, EARLY))
    pltpu.make_async_copy(late, late, local_sem.at[1]).wait()
    send_pieces(range(EARLY, NP))
    for g, e in ((0, 0), (1, 0), (0, 1), (2, 0), (3, 0), (1, 1), (2, 1), (3, 1)):
        load_win(e, g).start()

    def relay_b(*ks):
        for k in ks:
            with scope(f"relayb{k}"):
                @pl.when(lead)
                def _():
                    copy_b(k).wait_recv()
                    copy_c(k).start()
                    if k < TWO_WAY:
                        copy_d(k, tp).start()

    def relay_d(*ks):
        for k in ks:
            with scope(f"relayd{k}"):
                @pl.when(lead)
                def _():
                    copy_d(k, peer).wait_recv()
                    copy_e(k).start()

    scores = score[...]
    ltall[core] = ltsend[ep]
    grown = jnp.exp(scores - jnp.max(scores, axis=0, keepdims=True))
    probs[...] = grown / jnp.sum(grown, axis=0, keepdims=True)

    relay_b(0, 1)
    with scope("ltwait"):
        three = ltall.at[pl.ds(0, 3)]
        remote(three, three, 4, lt_r.at[0], to_near).wait_recv()

    below = jnp.where(lax.broadcasted_iota(jnp.int32, (128, 128), 0) < lax.broadcasted_iota(jnp.int32, (128, 128), 1),
                      1.0, 0.0).astype(BF16)
    before = jnp.where(lax.broadcasted_iota(jnp.int32, (8, 8), 1) < lax.broadcasted_iota(jnp.int32, (8, 8), 0),
                       1.0, 0.0).astype(BF16)

    first_half = lax.broadcasted_iota(jnp.int32, (HC, TOK), 0).astype(F32)

    def pick(i):
        line = jnp.concatenate([ltall[p, i:i + 1, :] for p in range(EP)], axis=1)
        rank = jnp.zeros((1, TOK), F32)
        for s in range(TOK // 128):
            wide = jnp.concatenate([column(line[:, s * 128:(s + 1) * 128])] * (TOK // 128), axis=1)
            rank = rank + jnp.sum(jnp.where(wide > line, 1.0, 0.0), axis=0, keepdims=True)
        taken = jnp.where(rank < CAP, 1.0, 0.0)
        grid = jnp.concatenate([taken[:, s * 128:(s + 1) * 128] for s in range(8)], axis=0)
        grid16 = grid.astype(BF16)
        inside = jnp.dot(grid16, below, preferred_element_type=F32)
        ahead = jnp.sum(jnp.dot(before, grid16, preferred_element_type=F32), axis=1, keepdims=True)
        slot = jnp.where(grid > 0.5, inside + ahead, -1.0)
        slots[core, i * 8:(i + 1) * 8, :] = slot
        slot = jnp.concatenate([slot[s:s + 1, :] for s in range(8)], axis=1)
        hot1[i * HC:(i + 1) * HC, :] = jnp.where(first_half[:, :3 * BLK] == slot[:, :3 * BLK], 1.0, 0.0).astype(BF16)

    def pick_late():
        for i in range(OWN):
            slot = jnp.concatenate([slots[core, i * 8 + s:i * 8 + s + 1, :] for s in range(8)], axis=1)
            hot2[i * HC:(i + 1) * HC, :] = jnp.where(first_half + HC == slot, 1.0, 0.0).astype(BF16)

    def cut(first_unit, units, place, places):
        part = pl.ds(place * BLK, places * BLK)
        return jnp.concatenate([xall[u, part, :] for u in range(first_unit, first_unit + units)], axis=1)

    def lanes_of(first_unit, units):
        return slice(first_unit * UNIT, (first_unit + units) * UNIT)

    def take_own(pairs):
        for u in pairs:
            xg[:, lanes_of(2 * u, 2)] = jnp.dot(hot1[:, :2 * BLK], cut(2 * u, 2, 0, 2), preferred_element_type=F32).astype(BF16)

    def take_a(e, units):
        mid = slice(e * HC, (e + 1) * HC)
        for u, n in units:
            cols = lanes_of(u, n)
            r = jnp.dot(hot1[mid, 2 * BLK:], cut(u, n, A, 1), preferred_element_type=F32)
            xg[mid, cols] = (xg[mid, cols].astype(F32) + r).astype(BF16)

    def first_tiles(h, e, first_unit, units, x, w_next=None):
        z = None
        for n in range(HID // TILE):
            cols = slice(n * TILE, (n + 1) * TILE)
            r = jnp.dot(x, win[e, first_unit * UNIT:(first_unit + units) * UNIT, cols], preferred_element_type=F32)
            if first_unit > 0:
                r = r + acc[e, :, cols]
            if first_unit + units < DIM // UNIT:
                acc[e, :, cols] = r
            else:
                part = gelu(r).astype(BF16)
                hid[h, e, :, cols] = part
                if w_next is not None:
                    step = jnp.dot(part, w_next[cols, :], preferred_element_type=F32)
                    z = step if z is None else z + step
        return z

    def first(e, first_unit, units, w_next=None):
        with scope(f"first{first_unit}e{e}"):
            for g in range(NG):
                if first_unit <= g * UG < first_unit + units:
                    wait_win(e, g)
            take_a(e, [(u, 2) for u in range(first_unit, first_unit + units, 2)])
            return first_tiles(0, e, first_unit, units, xg[e * HC:(e + 1) * HC, lanes_of(first_unit, units)], w_next)

    def first_late(g):
        for m in range(0, UG, 2):
            x = cut(UG * g + m, 2, 0, EP)
            xg2[:, m * UNIT:(m + 2) * UNIT] = jnp.dot(hot2[...], x, preferred_element_type=F32).astype(BF16)

        def body(e, _):
            first_tiles(1, e, UG * g, UG, xg2[pl.ds(pl.multiple_of(e * HC, HC), HC), :])
            return 0
        lax.fori_loop(0, OWN, body, 0)

    def second(m, r=None):
        h, j, e = order[m]
        n = h * NJ + j
        with scope(f"second{n}e{e}"):
            if m > 0:
                wait_wout(m)
            mid = slice(e * HC, (e + 1) * HC)
            if r is None:
                r = jnp.dot(hid[h, e], wout[m % NB], preferred_element_type=F32)
            snd[n, mid, :] = r[:, :NC]
            mine[n, mid, :] = r[:, NC:]
            copy_s(n, e).start()
            load_wout(m + NB)

    def ready(*ks):
        with scope(f"ready{ks[0]}"):
            @pl.when(follow)
            def _():
                for k in ks:
                    copy_c(k).wait_recv()
                    if k == NP - 1:
                        for g in range(NG):
                            copy_g(g).start()
                    if k < TWO_WAY:
                        copy_e(k).wait_recv()

    relay_b(2)
    with scope("pick0"):
        pick(0)
    relay_b(3)
    with scope("pick1"):
        pick(1)
    relay_b(4)
    with scope("wait_a"):
        near_x = xall.at[:, rows(place_near)]
        remote(near_x, near_x, 1, a_r.at[0], to_near).wait_recv()
    relay_d(0, 1)
    with scope("own0"):
        take_own(range(4))
    relay_b(5)
    with scope("own1"):
        take_own(range(4, 8))
    relay_d(2)
    relay_b(6)
    ready(0, 1, 2)
    first(0, 0, 4)
    for m in range(NB):
        load_wout(m)
    relay_b(7)
    relay_d(3, 4)
    ready(3, 4)
    first(0, 4, 4)
    relay_d(5)
    ready(5)
    first(0, 8, 2)
    relay_b(8)
    ready(8)
    first(0, 10, 2)
    relay_d(6)
    ready(6)
    first(0, 12, 2)
    wait_wout(0)
    relay_b(9)
    relay_d(7)
    ready(7, 9)
    second(0, first(0, 14, 2, wout.at[0]))
    for m in range(1, len(head)):
        second(m)
    first(1, 0, 4)
    first(1, 4, 4)
    first(1, 8, 4)
    first(1, 12, 4)
    copy_slots(to_near, core).start()
    copy_slots(to_far, there).start()
    copy_slots(to_diag, there).start()

    def relay_g(g):
        with scope(f"relayg{g}"):
            @pl.when(follow)
            def _():
                copy_g(g).wait_recv()
                copy_f(g).start()

    half = OWN * NJ
    for m in range(len(head), half):
        second(m)
        if m in (half - 8, half - 2):
            relay_g(0 if m == half - 8 else 1)
    with scope("pick_late"):
        pick_late()
    for g in range(NG):
        if g > 0 and g + 1 < NG:
            relay_g(g + 1)
        with scope(f"readyB{g}"):
            @pl.when(lead)
            def _():
                copy_f(g).wait_recv()
        with scope(f"firstB{g}"):
            first_late(g)
    def close(u):
        with scope(f"waits{u}"):
            wait_s(u)
        start, size = span(u)
        for n in range(start, start + size):
            zall[n, core] = (mine[n] + rcv[n]).astype(BF16)
        copy_zx(u, core, there).start()
        copy_zc(u, core).start()

    def forward(u):
        with scope(f"waitzx{u}"):
            copy_zx(u, place_far, place_far).wait_recv()
        copy_zf(u, place_far).start()

    def combine(j):
        total = jnp.zeros((BLK, NC), F32)
        for p in range(EP):
            for i in range(OWN):
                mid = slice(i * HC, (i + 1) * HC)
                z = jnp.concatenate([zall[j, p, mid, :], zall[NJ + j, p, mid, :]], axis=0)
                total = total + gate[p * OWN + i] * jnp.dot(back[p * OWN + i], z, preferred_element_type=F32)
        own = xall[tp * NJ + j, rows(core), :]
        res[j] = (own.astype(F32) + total).astype(BF16)
        copy_res(j, tp).start()
        out[:, pl.ds(pl.multiple_of(tp * HALF + j * NC, NC), NC)] = res[j]

    close(0)
    for m in range(half, 2 * half):
        second(m)


    with scope("slotwait"):
        three = slots.at[pl.ds(0, 3)]
        remote(three, three, 0, sl_r.at[0], to_near).wait_recv()
    with scope("back"):
        lanes = lax.broadcasted_iota(jnp.int32, (128, CAP), 1).astype(F32)
        for p in range(EP):
            mark = core if p < 2 else there
            owner = 2 * chip + p if p < 2 else 2 * (1 - chip) + (3 - p)
            for i in range(OWN):
                for c in range(BLK // 128):
                    part = slice(c * 128, (c + 1) * 128)
                    col = column(slots[p, pl.ds(i * 8 + mark * 2 + c, 1), :])
                    back[p * OWN + i, part, :] = jnp.where(jnp.concatenate([col, col], axis=1) == lanes, 1.0, 0.0).astype(BF16)
                    gate[p * OWN + i, part, :] = column(probs[pl.ds(owner * OWN + i, 1), :][:, part])

    units = len(SPANS)
    for u in range(1, units + 2):
        if u < units:
            close(u)
        if u - 1 < units:
            forward(u - 1)
        if u - 2 >= EARLY_SPANS:
            with scope(f"waitzn{u - 2}"):
                if u - 2 == EARLY_SPANS:
                    wait_zn(0)
                wait_zn(u - 2)
            start, size = span(u - 2)
            for n in range(start, start + size):
                combine(n - NJ)

    with scope("drain"):
        def left(ref, family):
            remote(ref, ref, family, res_r.at[0], to_near).wait_send()
        left(ltall.at[pl.ds(0, 3)], 4)
        left(slots.at[pl.ds(0, 3)], 0)
        left(zall.at[pl.ds(0, 12)], 1)
        left(zall.at[pl.ds(0, 12)], 2)
        left(zall.at[pl.ds(0, 10)], 3)
        remote(res, res, 3, res_r.at[0], to_peer).wait_recv()


def solution(mesh):
    def local_layer(tokens, logits, w_in, w_out):
        dma = pltpu.SemaphoreType.DMA
        units = len(SPANS)
        scratch = [
            pltpu.VMEM((DIM // UNIT, TOK, UNIT), BF16),
            pltpu.VMEM((EXPERTS, BLK), F32),
            pltpu.VMEM((EP, OWN, BLK), F32),
            pltpu.VMEM((EP, OWN, BLK), F32),
            pltpu.VMEM((EP, OWN * 8, 128), F32),
            pltpu.VMEM((OWN * HC, 3 * BLK), BF16),
            pltpu.VMEM((OWN * HC, TOK), BF16),
            pltpu.VMEM((OWN * HC, DIM), BF16),
            pltpu.VMEM((OWN * HC, KG), BF16),
            pltpu.VMEM((OWN, DIM, HID), BF16),
            pltpu.VMEM((OWN, HC, HID), F32),
            pltpu.VMEM((2, OWN, HC, HID), BF16),
            pltpu.VMEM((NB, HID, 2 * NC), BF16),
            pltpu.VMEM((2 * NJ, OWN * HC, NC), F32),
            pltpu.VMEM((2 * NJ, OWN * HC, NC), F32),
            pltpu.VMEM((2 * NJ, OWN * HC, NC), F32),
            pltpu.VMEM((2 * NJ, EP, OWN * HC, NC), BF16),
            pltpu.VMEM((EXPERTS, BLK, CAP), BF16),
            pltpu.VMEM((EXPERTS, BLK, NC), F32),
            pltpu.VMEM((EXPERTS, BLK), F32),
            pltpu.VMEM((NJ, BLK, NC), BF16),
            dma((3,)), dma((NG + 1,)), dma((NB,)), dma((5,)),
            dma((1,)), dma((1,)), dma((1,)), dma((NP,)), dma((TWO_WAY,)), dma((NG,)),
            dma((units,)), dma((units,)), dma((1 + units - EARLY_SPANS,)), dma((1,)),
        ]
        return pl.pallas_call(
            kernel,
            out_shape=pltpu.VMEM(tokens.shape, BF16),
            in_specs=[pl.BlockSpec(memory_space=pl.ANY), pl.BlockSpec(memory_space=pl.ANY),
                      pl.BlockSpec(memory_space=pl.ANY), pl.BlockSpec(memory_space=pl.ANY)],
            out_specs=pl.BlockSpec(memory_space=pltpu.VMEM),
            scratch_shapes=scratch,
            compiler_params=pltpu.CompilerParams(collective_id=0, has_side_effects=True,
                                                 vmem_limit_bytes=62_500_000),
            name="moe_layer",
        )(tokens, logits.T, w_in, w_out)

    row_spec = P(("dp", "ep"), None)
    return jax.shard_map(local_layer, mesh=mesh,
                         in_specs=(row_spec, row_spec, P("ep", None, "tp"), P("ep", "tp", None)),
                         out_specs=row_spec, check_vma=False)
```

```python
import jax
import jax.numpy as jnp
from jax import lax
from jax.experimental import pallas as pl
from jax.experimental.pallas import tpu as pltpu
from jax.sharding import PartitionSpec as P

MESH = pl.DeviceIdType.MESH
F32 = jnp.float32
BF16 = jnp.bfloat16

BLK = 256
XR = 128
YR = BLK - XR
EXPERTS = 8
OWN = 2
CAP = 256
HC = CAP // 2
DIM = 2048
HID = 2816
EP = 4
TOK = BLK * EP
HALF = DIM // 2
UNIT = 128
PIECES = [(0, 1), (1, 1), (2, 2), (4, 2), (6, 2), (8, 2), (12, 2), (14, 1), (10, 2), (15, 1)]
TWO_WAY = 8
NP = len(PIECES)
NG = 4
KG = DIM // NG
UG = KG // UNIT
NJ = 8
NC = HALF // NJ
SPANS = [(0, 4), (4, 4), (8, 2), (10, 2), (12, 2), (14, 1), (15, 1)]
EARLY_SPANS = 2
NB = 6
TILE = 256
EARLY = 3
EARLY_UNITS = 4


def gelu(v):
    return 0.5 * v * (1.0 + jnp.tanh(v * (0.7978845608028654 + 0.035677408136300125 * (v * v))))


def column(row):
    return jnp.transpose(jnp.broadcast_to(row, (128, 128)))


def kernel(tok, lt, w_in, w_out, out,
           xall, score, ltsend, ltall, slots, hot1, hot2, xg, xg2, win, acc, hid, wout, snd, mine, rcv, zall, back, gate, probs, res, passed,
           local_sem, win_sem, wout_sem, send, lt_r, sl_r, a_r, bc_r, de_r, gf_r, s_r, zx_r, zn_r, res_r, pass_r):
    scope = jax.named_scope
    ep = lax.axis_index("ep")
    tp = lax.axis_index("tp")
    core = lax.rem(ep, 2)
    chip = ep // 2
    near = ep + 1 - 2 * core
    far = lax.rem(ep + 2, 4)
    diag = 3 - ep
    peer = 1 - tp
    to_near, to_far, to_diag = {"ep": near, "tp": tp}, {"ep": far, "tp": tp}, {"ep": diag, "tp": tp}
    to_peer = {"ep": ep, "tp": peer}
    to_near_peer = {"ep": near, "tp": peer}
    A, B = 2, 3
    place_near, place_far, place_diag = 1 - core, 3 - core, 2 + core
    there = 3 - core
    lead, follow = core == 1, core == 0

    def rows(place, offset=0, size=BLK):
        return pl.ds(pl.multiple_of(place * BLK + offset, 32), size)

    def remote(src, dst, family, recv, where):
        return pltpu.make_async_remote_copy(src_ref=src, dst_ref=dst, send_sem=send.at[family], recv_sem=recv,
                                            device_id=where, device_id_type=MESH)

    def load_tok(k):
        return pltpu.make_async_copy(tok.at[:, pl.ds(k * UNIT, UNIT)], xall.at[k, rows(core)], local_sem.at[0 if k < EARLY_UNITS else 1])

    def load_win(e, g):
        part = pl.ds(g * KG, KG)
        return pltpu.make_async_copy(w_in.at[e, part], win.at[e, part], win_sem.at[min(g, 1) if e == 0 else 2])

    def wait_win(e, g):
        if e == 0 and g == 0:
            load_win(e, g).wait()
        elif e == 0 and g == 1:
            rest = win.at[e, pl.ds(KG, DIM - KG)]
            pltpu.make_async_copy(rest, rest, win_sem.at[1]).wait()
        elif g == 0:
            pltpu.make_async_copy(win.at[e], win.at[e], win_sem.at[2]).wait()

    head = [(0, j, 0) for j in range(4)]
    order = head + [(0, j, 1) for j in range(4)]
    order += [(0, j, e) for j in range(4, NJ) for e in range(OWN)] + [(1, j, e) for j in range(NJ) for e in range(OWN)]

    def load_wout(m):
        if m >= len(order):
            return
        _, j, e = order[m]
        for side, half in enumerate((peer, tp)):
            cols = pl.ds(pl.multiple_of(half * HALF + j * NC, NC), NC)
            pltpu.make_async_copy(w_out.at[e, :, cols], wout.at[m % NB, :, pl.ds(side * NC, NC)], wout_sem.at[m % NB]).start()

    def wait_wout(m):
        both = wout.at[m % NB]
        pltpu.make_async_copy(both, both, wout_sem.at[m % NB]).wait()

    def copy_lt(where, target, place):
        return remote(ltsend.at[target], ltall.at[place], 4, lt_r.at[0], where)

    def copy_slots(where, place):
        return remote(slots.at[core], slots.at[place], 0, sl_r.at[0], where)

    def copy_a(k, place):
        piece = xall.at[pl.ds(*PIECES[k]), rows(place)]
        return remote(piece, piece, 1, a_r.at[0], to_near)

    def b_rows(k, place):
        return rows(place, tp * YR, XR) if k < TWO_WAY else rows(place)

    def copy_b(k):
        units = pl.ds(*PIECES[k])
        return remote(xall.at[units, b_rows(k, core)], xall.at[units, b_rows(k, A)], 1, bc_r.at[k], to_far)

    def copy_c(k):
        piece = xall.at[pl.ds(*PIECES[k]), b_rows(k, A)]
        return remote(piece, piece, 1, bc_r.at[k], to_near)

    def copy_d(k, half):
        piece = xall.at[pl.ds(*PIECES[k]), rows(A, half * XR, YR)]
        return remote(piece, piece, 1, de_r.at[k], to_peer)

    def copy_e(k):
        piece = xall.at[pl.ds(*PIECES[k]), rows(A, peer * XR, YR)]
        return remote(piece, piece, 1, de_r.at[k], to_near)

    def copy_g(g):
        group = pl.ds(UG * g, UG)
        return remote(xall.at[group, rows(core)], xall.at[group, rows(B)], 1, gf_r.at[g], to_far)

    def copy_f(g):
        group = xall.at[pl.ds(UG * g, UG), rows(B)]
        return remote(group, group, 1, gf_r.at[g], to_near)

    def span(u):
        return SPANS[u]

    def unit(n):
        return [u for u, (start, size) in enumerate(SPANS) if start <= n < start + size][0]

    def copy_s(n, e):
        mid = pl.ds(e * HC, HC)
        return remote(snd.at[n, mid], rcv.at[n, mid], 3, s_r.at[unit(n)], to_peer)

    def wait_s(u):
        whole = rcv.at[pl.ds(*span(u))]
        remote(whole, whole, 3, s_r.at[u], to_peer).wait_recv()

    def copy_zc(u, place):
        part = zall.at[pl.ds(*span(u)), place]
        return remote(part, part, 2, zn_r.at[max(0, u - EARLY_SPANS + 1)], to_near)

    def copy_zf(u, place):
        part = zall.at[pl.ds(*span(u)), place]
        return remote(part, part, 2, zn_r.at[max(0, u - EARLY_SPANS + 1)], to_near)

    def wait_zn(u):
        start, size = SPANS[u] if u >= EARLY_SPANS else (0, NJ)
        whole = zall.at[pl.ds(start, size), pl.ds(0, 2)]
        remote(whole, whole, 2, zn_r.at[max(0, u - EARLY_SPANS + 1)], to_near).wait_recv()

    def copy_zx(u, src, dst):
        ns = pl.ds(*span(u))
        return remote(zall.at[ns, src], zall.at[ns, dst], 2, zx_r.at[u], to_far)

    def out_cols(half, j):
        return out.at[:, pl.ds(pl.multiple_of(half * HALF + j * NC, NC), NC)]

    def copy_res(j, half):
        return remote(res.at[j], out_cols(half, j), 3, res_r.at[0], to_peer)

    def copy_pass():
        return remote(res.at[0], passed, 3, pass_r.at[0], to_near)

    def copy_passed():
        return remote(passed, out_cols(tp, 0), 5, res_r.at[0], to_near_peer)

    barrier = pltpu.get_barrier_semaphore()
    for where in (to_near, to_far, to_diag, to_peer):
        pl.semaphore_signal(barrier, inc=1, device_id=where, device_id_type=MESH)
    load_lt = pltpu.make_async_copy(lt, score, local_sem.at[2])
    load_lt.start()
    for k in range(DIM // UNIT):
        load_tok(k).start()
    mine_x = xall.at[:, rows(core)]
    load_lt.wait()
    for d in range(EP):
        ltsend[d] = score[d * OWN:(d + 1) * OWN, :]
    early, late = (xall.at[pl.ds(a, n), rows(core)] for a, n in ((0, EARLY_UNITS), (EARLY_UNITS, DIM // UNIT - EARLY_UNITS)))
    pltpu.make_async_copy(early, early, local_sem.at[0]).wait()
    with scope("barrier"):
        pl.semaphore_wait(barrier, 4)

    def send_pieces(ks):
        @pl.when(lead)
        def _():
            for k in ks:
                copy_b(k).start()
        for k in ks:
            copy_a(k, core).start()

    send_pieces(range(1))
    copy_lt(to_near, near, core).start()
    copy_lt(to_far, far, there).start()
    copy_lt(to_diag, diag, there).start()
    send_pieces(range(1, EARLY))
    pltpu.make_async_copy(late, late, local_sem.at[1]).wait()
    send_pieces(range(EARLY, NP))
    for e in range(OWN):
        for g in range(NG):
            load_win(e, g).start()

    def relay_b(*ks):
        for k in ks:
            with scope(f"relayb{k}"):
                @pl.when(lead)
                def _():
                    copy_b(k).wait_recv()
                    copy_c(k).start()
                    if k < TWO_WAY:
                        copy_d(k, tp).start()

    def relay_d(*ks):
        for k in ks:
            with scope(f"relayd{k}"):
                @pl.when(lead)
                def _():
                    copy_d(k, peer).wait_recv()
                    copy_e(k).start()

    scores = score[...]
    ltall[core] = ltsend[ep]
    grown = jnp.exp(scores - jnp.max(scores, axis=0, keepdims=True))
    probs[...] = grown / jnp.sum(grown, axis=0, keepdims=True)

    relay_b(0, 1)
    with scope("ltwait"):
        three = ltall.at[pl.ds(0, 3)]
        remote(three, three, 4, lt_r.at[0], to_near).wait_recv()

    below = jnp.where(lax.broadcasted_iota(jnp.int32, (128, 128), 0) < lax.broadcasted_iota(jnp.int32, (128, 128), 1),
                      1.0, 0.0).astype(BF16)
    before = jnp.where(lax.broadcasted_iota(jnp.int32, (8, 8), 1) < lax.broadcasted_iota(jnp.int32, (8, 8), 0),
                       1.0, 0.0).astype(BF16)

    first_half = lax.broadcasted_iota(jnp.int32, (HC, TOK), 0).astype(F32)

    def pick(i):
        line = jnp.concatenate([ltall[p, i:i + 1, :] for p in range(EP)], axis=1)
        rank = jnp.zeros((1, TOK), F32)
        for s in range(TOK // 128):
            wide = jnp.concatenate([column(line[:, s * 128:(s + 1) * 128])] * (TOK // 128), axis=1)
            rank = rank + jnp.sum(jnp.where(wide > line, 1.0, 0.0), axis=0, keepdims=True)
        taken = jnp.where(rank < CAP, 1.0, 0.0)
        grid = jnp.concatenate([taken[:, s * 128:(s + 1) * 128] for s in range(8)], axis=0)
        grid16 = grid.astype(BF16)
        inside = jnp.dot(grid16, below, preferred_element_type=F32)
        ahead = jnp.sum(jnp.dot(before, grid16, preferred_element_type=F32), axis=1, keepdims=True)
        slot = jnp.where(grid > 0.5, inside + ahead, -1.0)
        slots[core, i * 8:(i + 1) * 8, :] = slot
        slot = jnp.concatenate([slot[s:s + 1, :] for s in range(8)], axis=1)
        hot1[i * HC:(i + 1) * HC, :] = jnp.where(first_half[:, :3 * BLK] == slot[:, :3 * BLK], 1.0, 0.0).astype(BF16)

    def pick_late():
        for i in range(OWN):
            slot = jnp.concatenate([slots[core, i * 8 + s:i * 8 + s + 1, :] for s in range(8)], axis=1)
            hot2[i * HC:(i + 1) * HC, :] = jnp.where(first_half + HC == slot, 1.0, 0.0).astype(BF16)

    def cut(first_unit, units, place, places):
        part = pl.ds(place * BLK, places * BLK)
        return jnp.concatenate([xall[u, part, :] for u in range(first_unit, first_unit + units)], axis=1)

    def lanes_of(first_unit, units):
        return slice(first_unit * UNIT, (first_unit + units) * UNIT)

    def take_own(pairs):
        for u in pairs:
            xg[:, lanes_of(2 * u, 2)] = jnp.dot(hot1[:, :2 * BLK], cut(2 * u, 2, 0, 2), preferred_element_type=F32).astype(BF16)

    def take_a(e, units):
        mid = slice(e * HC, (e + 1) * HC)
        for u, n in units:
            cols = lanes_of(u, n)
            r = jnp.dot(hot1[mid, 2 * BLK:], cut(u, n, A, 1), preferred_element_type=F32)
            xg[mid, cols] = (xg[mid, cols].astype(F32) + r).astype(BF16)

    def first_tiles(h, e, first_unit, units, x, w_next=None):
        z = None
        for n in range(HID // TILE):
            cols = slice(n * TILE, (n + 1) * TILE)
            r = jnp.dot(x, win[e, first_unit * UNIT:(first_unit + units) * UNIT, cols], preferred_element_type=F32)
            if first_unit > 0:
                r = r + acc[e, :, cols]
            if first_unit + units < DIM // UNIT:
                acc[e, :, cols] = r
            else:
                part = gelu(r).astype(BF16)
                hid[h, e, :, cols] = part
                if w_next is not None:
                    step = jnp.dot(part, w_next[cols, :], preferred_element_type=F32)
                    z = step if z is None else z + step
        return z

    def first(e, first_unit, units, w_next=None):
        with scope(f"first{first_unit}e{e}"):
            for g in range(NG):
                if first_unit <= g * UG < first_unit + units:
                    wait_win(e, g)
            take_a(e, [(u, 2) for u in range(first_unit, first_unit + units, 2)])
            return first_tiles(0, e, first_unit, units, xg[e * HC:(e + 1) * HC, lanes_of(first_unit, units)], w_next)

    def first_late(g):
        for m in range(0, UG, 2):
            x = cut(UG * g + m, 2, 0, EP)
            xg2[:, m * UNIT:(m + 2) * UNIT] = jnp.dot(hot2[...], x, preferred_element_type=F32).astype(BF16)

        def body(e, _):
            first_tiles(1, e, UG * g, UG, xg2[pl.ds(pl.multiple_of(e * HC, HC), HC), :])
            return 0
        lax.fori_loop(0, OWN, body, 0)

    def second(m, r=None):
        h, j, e = order[m]
        n = h * NJ + j
        with scope(f"second{n}e{e}"):
            if m > 0:
                wait_wout(m)
            mid = slice(e * HC, (e + 1) * HC)
            if r is None:
                r = jnp.dot(hid[h, e], wout[m % NB], preferred_element_type=F32)
            snd[n, mid, :] = r[:, :NC]
            mine[n, mid, :] = r[:, NC:]
            copy_s(n, e).start()
            load_wout(m + NB)

    def ready(*ks):
        with scope(f"ready{ks[0]}"):
            @pl.when(follow)
            def _():
                for k in ks:
                    copy_c(k).wait_recv()
                    if k == NP - 1:
                        for g in range(NG):
                            copy_g(g).start()
                    if k < TWO_WAY:
                        copy_e(k).wait_recv()

    relay_b(2)
    with scope("pick0"):
        pick(0)
    relay_b(3)
    with scope("pick1"):
        pick(1)
    relay_b(4)
    with scope("wait_a"):
        near_x = xall.at[:, rows(place_near)]
        remote(near_x, near_x, 1, a_r.at[0], to_near).wait_recv()
    relay_d(0, 1)
    with scope("own0"):
        take_own(range(4))
    relay_b(5)
    with scope("own1"):
        take_own(range(4, 8))
    relay_d(2)
    relay_b(6)
    ready(0, 1, 2)
    first(0, 0, 4)
    for m in range(NB):
        load_wout(m)
    relay_b(7)
    relay_d(3, 4)
    ready(3, 4)
    first(0, 4, 4)
    relay_d(5)
    ready(5)
    first(0, 8, 2)
    relay_b(8)
    ready(8)
    first(0, 10, 2)
    relay_d(6)
    ready(6)
    first(0, 12, 2)
    wait_wout(0)
    relay_b(9)
    relay_d(7)
    ready(7, 9)
    second(0, first(0, 14, 2, wout.at[0]))
    for m in range(1, len(head)):
        second(m)
    first(1, 0, 4)
    first(1, 4, 4)
    first(1, 8, 4)
    first(1, 12, 4)
    copy_slots(to_near, core).start()
    copy_slots(to_far, there).start()
    copy_slots(to_diag, there).start()

    def relay_g(g):
        with scope(f"relayg{g}"):
            @pl.when(follow)
            def _():
                copy_g(g).wait_recv()
                copy_f(g).start()

    half = OWN * NJ
    for m in range(len(head), half):
        second(m)
        if m in (half - 8, half - 2):
            relay_g(0 if m == half - 8 else 1)
    with scope("pick_late"):
        pick_late()
    for g in range(NG):
        if g > 0 and g + 1 < NG:
            relay_g(g + 1)
        with scope(f"readyB{g}"):
            @pl.when(lead)
            def _():
                copy_f(g).wait_recv()
        with scope(f"firstB{g}"):
            first_late(g)
    def close(u):
        with scope(f"waits{u}"):
            wait_s(u)
        start, size = span(u)
        for n in range(start, start + size):
            zall[n, core] = (mine[n] + rcv[n]).astype(BF16)
        copy_zx(u, core, there).start()
        copy_zc(u, core).start()

    def forward(u):
        with scope(f"waitzx{u}"):
            copy_zx(u, place_far, place_far).wait_recv()
        copy_zf(u, place_far).start()

    def combine(j):
        total = jnp.zeros((BLK, NC), F32)
        for p in range(EP):
            for i in range(OWN):
                mid = slice(i * HC, (i + 1) * HC)
                z = jnp.concatenate([zall[j, p, mid, :], zall[NJ + j, p, mid, :]], axis=0)
                total = total + gate[p * OWN + i] * jnp.dot(back[p * OWN + i], z, preferred_element_type=F32)
        own = xall[tp * NJ + j, rows(core), :]
        res[j] = (own.astype(F32) + total).astype(BF16)
        if j > 0:
            copy_res(j, tp).start()
        else:
            @pl.when(lead)
            def _():
                copy_res(j, tp).start()

            @pl.when(follow)
            def _():
                copy_pass().start()
        out[:, pl.ds(pl.multiple_of(tp * HALF + j * NC, NC), NC)] = res[j]

    close(0)
    for m in range(half, 2 * half):
        second(m)


    with scope("slotwait"):
        three = slots.at[pl.ds(0, 3)]
        remote(three, three, 0, sl_r.at[0], to_near).wait_recv()
    with scope("back"):
        lanes = lax.broadcasted_iota(jnp.int32, (128, CAP), 1).astype(F32)
        for p in range(EP):
            mark = core if p < 2 else there
            owner = 2 * chip + p if p < 2 else 2 * (1 - chip) + (3 - p)
            for i in range(OWN):
                for c in range(BLK // 128):
                    part = slice(c * 128, (c + 1) * 128)
                    col = column(slots[p, pl.ds(i * 8 + mark * 2 + c, 1), :])
                    back[p * OWN + i, part, :] = jnp.where(jnp.concatenate([col, col], axis=1) == lanes, 1.0, 0.0).astype(BF16)
                    gate[p * OWN + i, part, :] = column(probs[pl.ds(owner * OWN + i, 1), :][:, part])

    units = len(SPANS)
    for u in range(1, units + 2):
        if u < units:
            close(u)
        if u - 1 < units:
            forward(u - 1)
        if u - 2 >= EARLY_SPANS:
            with scope(f"waitzn{u - 2}"):
                if u - 2 == EARLY_SPANS:
                    wait_zn(0)
                wait_zn(u - 2)
            start, size = span(u - 2)
            for n in range(start, start + size):
                combine(n - NJ)
            if u - 2 == EARLY_SPANS + 1:
                @pl.when(lead)
                def _():
                    copy_pass().wait_recv()
                    copy_passed().start()

    with scope("drain"):
        def left(ref, family):
            remote(ref, ref, family, res_r.at[0], to_near).wait_send()
        left(ltall.at[pl.ds(0, 3)], 4)
        left(slots.at[pl.ds(0, 3)], 0)
        left(zall.at[pl.ds(0, 12)], 1)
        left(zall.at[pl.ds(0, 12)], 2)
        left(zall.at[pl.ds(0, 10)], 3)

        @pl.when(lead)
        def _():
            left(passed, 5)
        remote(res, res, 3, res_r.at[0], to_peer).wait_recv()


def solution(mesh):
    def local_layer(tokens, logits, w_in, w_out):
        dma = pltpu.SemaphoreType.DMA
        units = len(SPANS)
        scratch = [
            pltpu.VMEM((DIM // UNIT, TOK, UNIT), BF16),
            pltpu.VMEM((EXPERTS, BLK), F32),
            pltpu.VMEM((EP, OWN, BLK), F32),
            pltpu.VMEM((EP, OWN, BLK), F32),
            pltpu.VMEM((EP, OWN * 8, 128), F32),
            pltpu.VMEM((OWN * HC, 3 * BLK), BF16),
            pltpu.VMEM((OWN * HC, TOK), BF16),
            pltpu.VMEM((OWN * HC, DIM), BF16),
            pltpu.VMEM((OWN * HC, KG), BF16),
            pltpu.VMEM((OWN, DIM, HID), BF16),
            pltpu.VMEM((OWN, HC, HID), F32),
            pltpu.VMEM((2, OWN, HC, HID), BF16),
            pltpu.VMEM((NB, HID, 2 * NC), BF16),
            pltpu.VMEM((2 * NJ, OWN * HC, NC), F32),
            pltpu.VMEM((2 * NJ, OWN * HC, NC), F32),
            pltpu.VMEM((2 * NJ, OWN * HC, NC), F32),
            pltpu.VMEM((2 * NJ, EP, OWN * HC, NC), BF16),
            pltpu.VMEM((EXPERTS, BLK, CAP), BF16),
            pltpu.VMEM((EXPERTS, BLK, NC), F32),
            pltpu.VMEM((EXPERTS, BLK), F32),
            pltpu.VMEM((NJ, BLK, NC), BF16),
            pltpu.VMEM((BLK, NC), BF16),
            dma((3,)), dma((3,)), dma((NB,)), dma((6,)),
            dma((1,)), dma((1,)), dma((1,)), dma((NP,)), dma((TWO_WAY,)), dma((NG,)),
            dma((units,)), dma((units,)), dma((1 + units - EARLY_SPANS,)), dma((1,)), dma((1,)),
        ]
        return pl.pallas_call(
            kernel,
            out_shape=pltpu.VMEM(tokens.shape, BF16),
            in_specs=[pl.BlockSpec(memory_space=pl.ANY), pl.BlockSpec(memory_space=pl.ANY),
                      pl.BlockSpec(memory_space=pl.ANY), pl.BlockSpec(memory_space=pl.ANY)],
            out_specs=pl.BlockSpec(memory_space=pltpu.VMEM),
            scratch_shapes=scratch,
            compiler_params=pltpu.CompilerParams(collective_id=0, has_side_effects=True,
                                                 vmem_limit_bytes=62_500_000),
            name="moe_layer",
        )(tokens, logits.T, w_in, w_out)

    row_spec = P(("dp", "ep"), None)
    return jax.shard_map(local_layer, mesh=mesh,
                         in_specs=(row_spec, row_spec, P("ep", None, "tp"), P("ep", "tp", None)),
                         out_specs=row_spec, check_vma=False)
```

```python
import jax
import jax.numpy as jnp
from jax import lax
from jax.experimental import pallas as pl
from jax.experimental.pallas import tpu as pltpu
from jax.sharding import PartitionSpec as P

MESH = pl.DeviceIdType.MESH
F32 = jnp.float32
BF16 = jnp.bfloat16

BLK = 256
XR = 128
YR = BLK - XR
EXPERTS = 8
OWN = 2
CAP = 256
HC = CAP // 2
DIM = 2048
HID = 2816
EP = 4
TOK = BLK * EP
HALF = DIM // 2
UNIT = 128
PIECES = [(0, 1), (1, 1), (2, 2), (4, 2), (6, 2), (8, 2), (12, 2), (14, 1), (10, 2), (15, 1)]
TWO_WAY = 8
NP = len(PIECES)
NG = 4
KG = DIM // NG
UG = KG // UNIT
NJ = 8
NC = HALF // NJ
SPANS = [(0, 4), (4, 4), (8, 2), (10, 2), (12, 2), (14, 1), (15, 1)]
EARLY_SPANS = 2
NB = 6
TILE = 256
EARLY = 3
EARLY_UNITS = 4


def gelu(v):
    return 0.5 * v * (1.0 + jnp.tanh(v * (0.7978845608028654 + 0.035677408136300125 * (v * v))))


def column(row):
    return jnp.transpose(jnp.broadcast_to(row, (128, 128)))


def kernel(tok, lt, w_in, w_out, out,
           xall, score, ltsend, ltall, slots, hot1, hot2, xg, xg2, win, acc, hid, wout, snd, mine, rcv, zall, back, gate, probs, res, passed,
           local_sem, win_sem, wout_sem, send, lt_r, sl_r, a_r, bc_r, de_r, gf_r, s_r, zx_r, zn_r, res_r, pass_r):
    scope = jax.named_scope
    ep = lax.axis_index("ep")
    tp = lax.axis_index("tp")
    core = lax.rem(ep, 2)
    chip = ep // 2
    near = ep + 1 - 2 * core
    far = lax.rem(ep + 2, 4)
    diag = 3 - ep
    peer = 1 - tp
    to_near, to_far, to_diag = {"ep": near, "tp": tp}, {"ep": far, "tp": tp}, {"ep": diag, "tp": tp}
    to_peer = {"ep": ep, "tp": peer}
    to_near_peer = {"ep": near, "tp": peer}
    A, B = 2, 3
    place_near, place_far, place_diag = 1 - core, 3 - core, 2 + core
    there = 3 - core
    lead, follow = core == 1, core == 0

    def rows(place, offset=0, size=BLK):
        return pl.ds(pl.multiple_of(place * BLK + offset, 32), size)

    def remote(src, dst, family, recv, where):
        return pltpu.make_async_remote_copy(src_ref=src, dst_ref=dst, send_sem=send.at[family], recv_sem=recv,
                                            device_id=where, device_id_type=MESH)

    def load_tok(k):
        return pltpu.make_async_copy(tok.at[:, pl.ds(k * UNIT, UNIT)], xall.at[k, rows(core)], local_sem.at[0 if k < EARLY_UNITS else 1])

    def load_win(e, g):
        part = pl.ds(g * KG, KG)
        return pltpu.make_async_copy(w_in.at[e, part], win.at[e, part], win_sem.at[min(g, 1) if e == 0 else 2])

    def wait_win(e, g):
        if e == 0 and g == 0:
            load_win(e, g).wait()
        elif e == 0 and g == 1:
            rest = win.at[e, pl.ds(KG, DIM - KG)]
            pltpu.make_async_copy(rest, rest, win_sem.at[1]).wait()
        elif g == 0:
            pltpu.make_async_copy(win.at[e], win.at[e], win_sem.at[2]).wait()

    head = [(0, j, 0) for j in range(4)]
    order = head + [(0, j, 1) for j in range(4)]
    order += [(0, j, e) for j in range(4, NJ) for e in range(OWN)] + [(1, j, e) for j in range(NJ) for e in range(OWN)]

    def load_wout(m):
        if m >= len(order):
            return
        _, j, e = order[m]
        for side, half in enumerate((peer, tp)):
            cols = pl.ds(pl.multiple_of(half * HALF + j * NC, NC), NC)
            pltpu.make_async_copy(w_out.at[e, :, cols], wout.at[m % NB, :, pl.ds(side * NC, NC)], wout_sem.at[m % NB]).start()

    def wait_wout(m):
        both = wout.at[m % NB]
        pltpu.make_async_copy(both, both, wout_sem.at[m % NB]).wait()

    def copy_lt(where, target, place):
        return remote(ltsend.at[target], ltall.at[place], 4, lt_r.at[0], where)

    def copy_slots(where, place):
        return remote(slots.at[core], slots.at[place], 0, sl_r.at[0], where)

    def copy_a(k, place):
        piece = xall.at[pl.ds(*PIECES[k]), rows(place)]
        return remote(piece, piece, 1, a_r.at[0], to_near)

    def b_rows(k, place):
        return rows(place, tp * YR, XR) if k < TWO_WAY else rows(place)

    def copy_b(k):
        units = pl.ds(*PIECES[k])
        return remote(xall.at[units, b_rows(k, core)], xall.at[units, b_rows(k, A)], 1, bc_r.at[k], to_far)

    def copy_c(k):
        piece = xall.at[pl.ds(*PIECES[k]), b_rows(k, A)]
        return remote(piece, piece, 1, bc_r.at[k], to_near)

    def copy_d(k, half):
        piece = xall.at[pl.ds(*PIECES[k]), rows(A, half * XR, YR)]
        return remote(piece, piece, 1, de_r.at[k], to_peer)

    def copy_e(k):
        piece = xall.at[pl.ds(*PIECES[k]), rows(A, peer * XR, YR)]
        return remote(piece, piece, 1, de_r.at[k], to_near)

    def copy_g(g):
        group = pl.ds(UG * g, UG)
        return remote(xall.at[group, rows(core)], xall.at[group, rows(B)], 1, gf_r.at[g], to_far)

    def copy_f(g):
        group = xall.at[pl.ds(UG * g, UG), rows(B)]
        return remote(group, group, 1, gf_r.at[g], to_near)

    def span(u):
        return SPANS[u]

    def unit(n):
        return [u for u, (start, size) in enumerate(SPANS) if start <= n < start + size][0]

    def copy_s(n, e):
        mid = pl.ds(e * HC, HC)
        return remote(snd.at[n, mid], rcv.at[n, mid], 3, s_r.at[unit(n)], to_peer)

    def wait_s(u):
        whole = rcv.at[pl.ds(*span(u))]
        remote(whole, whole, 3, s_r.at[u], to_peer).wait_recv()

    def copy_zc(u, place):
        part = zall.at[pl.ds(*span(u)), place]
        return remote(part, part, 2, zn_r.at[max(0, u - EARLY_SPANS + 1)], to_near)

    def copy_zf(u, place):
        part = zall.at[pl.ds(*span(u)), place]
        return remote(part, part, 2, zn_r.at[max(0, u - EARLY_SPANS + 1)], to_near)

    def wait_zn(u):
        start, size = SPANS[u] if u >= EARLY_SPANS else (0, NJ)
        whole = zall.at[pl.ds(start, size), pl.ds(0, 2)]
        remote(whole, whole, 2, zn_r.at[max(0, u - EARLY_SPANS + 1)], to_near).wait_recv()

    def copy_zx(u, src, dst):
        ns = pl.ds(*span(u))
        return remote(zall.at[ns, src], zall.at[ns, dst], 2, zx_r.at[u], to_far)

    def out_cols(half, j):
        return out.at[:, pl.ds(pl.multiple_of(half * HALF + j * NC, NC), NC)]

    def copy_res(j, half):
        return remote(res.at[j], out_cols(half, j), 3, res_r.at[0], to_peer)

    def copy_pass():
        return remote(res.at[0], passed, 3, pass_r.at[0], to_near)

    def copy_passed():
        return remote(passed, out_cols(tp, 0), 5, res_r.at[0], to_near_peer)

    barrier = pltpu.get_barrier_semaphore()
    for where in (to_near, to_far, to_diag, to_peer):
        pl.semaphore_signal(barrier, inc=1, device_id=where, device_id_type=MESH)
    load_lt = pltpu.make_async_copy(lt, score, local_sem.at[2])
    load_lt.start()
    for k in range(DIM // UNIT):
        load_tok(k).start()
    mine_x = xall.at[:, rows(core)]
    load_lt.wait()
    for d in range(EP):
        ltsend[d] = score[d * OWN:(d + 1) * OWN, :]
    early, late = (xall.at[pl.ds(a, n), rows(core)] for a, n in ((0, EARLY_UNITS), (EARLY_UNITS, DIM // UNIT - EARLY_UNITS)))
    pltpu.make_async_copy(early, early, local_sem.at[0]).wait()
    with scope("barrier"):
        pl.semaphore_wait(barrier, 4)

    def send_pieces(ks):
        @pl.when(lead)
        def _():
            for k in ks:
                copy_b(k).start()
        for k in ks:
            copy_a(k, core).start()

    send_pieces(range(1))
    copy_lt(to_near, near, core).start()
    copy_lt(to_far, far, there).start()
    copy_lt(to_diag, diag, there).start()
    send_pieces(range(1, EARLY))
    pltpu.make_async_copy(late, late, local_sem.at[1]).wait()
    send_pieces(range(EARLY, NP))
    for e in range(OWN):
        for g in range(NG):
            load_win(e, g).start()

    def relay_b(*ks):
        for k in ks:
            with scope(f"relayb{k}"):
                @pl.when(lead)
                def _():
                    copy_b(k).wait_recv()
                    copy_c(k).start()
                    if k < TWO_WAY:
                        copy_d(k, tp).start()

    def relay_d(*ks):
        for k in ks:
            with scope(f"relayd{k}"):
                @pl.when(lead)
                def _():
                    copy_d(k, peer).wait_recv()
                    copy_e(k).start()

    scores = score[...]
    ltall[core] = ltsend[ep]
    grown = jnp.exp(scores - jnp.max(scores, axis=0, keepdims=True))
    probs[...] = grown / jnp.sum(grown, axis=0, keepdims=True)

    relay_b(0, 1)
    with scope("ltwait"):
        three = ltall.at[pl.ds(0, 3)]
        remote(three, three, 4, lt_r.at[0], to_near).wait_recv()

    below = jnp.where(lax.broadcasted_iota(jnp.int32, (128, 128), 0) < lax.broadcasted_iota(jnp.int32, (128, 128), 1),
                      1.0, 0.0).astype(BF16)
    before = jnp.where(lax.broadcasted_iota(jnp.int32, (8, 8), 1) < lax.broadcasted_iota(jnp.int32, (8, 8), 0),
                       1.0, 0.0).astype(BF16)

    first_half = lax.broadcasted_iota(jnp.int32, (HC, TOK), 0).astype(F32)

    def pick(i):
        line = jnp.concatenate([ltall[p, i:i + 1, :] for p in range(EP)], axis=1)
        rank = jnp.zeros((1, TOK), F32)
        for s in range(TOK // 128):
            wide = jnp.concatenate([column(line[:, s * 128:(s + 1) * 128])] * (TOK // 128), axis=1)
            rank = rank + jnp.sum(jnp.where(wide > line, 1.0, 0.0), axis=0, keepdims=True)
        taken = jnp.where(rank < CAP, 1.0, 0.0)
        grid = jnp.concatenate([taken[:, s * 128:(s + 1) * 128] for s in range(8)], axis=0)
        grid16 = grid.astype(BF16)
        inside = jnp.dot(grid16, below, preferred_element_type=F32)
        ahead = jnp.sum(jnp.dot(before, grid16, preferred_element_type=F32), axis=1, keepdims=True)
        slot = jnp.where(grid > 0.5, inside + ahead, -1.0)
        slots[core, i * 8:(i + 1) * 8, :] = slot
        slot = jnp.concatenate([slot[s:s + 1, :] for s in range(8)], axis=1)
        hot1[i * HC:(i + 1) * HC, :] = jnp.where(first_half[:, :3 * BLK] == slot[:, :3 * BLK], 1.0, 0.0).astype(BF16)

    def pick_late():
        for i in range(OWN):
            slot = jnp.concatenate([slots[core, i * 8 + s:i * 8 + s + 1, :] for s in range(8)], axis=1)
            hot2[i * HC:(i + 1) * HC, :] = jnp.where(first_half + HC == slot, 1.0, 0.0).astype(BF16)

    def cut(first_unit, units, place, places):
        part = pl.ds(place * BLK, places * BLK)
        return jnp.concatenate([xall[u, part, :] for u in range(first_unit, first_unit + units)], axis=1)

    def lanes_of(first_unit, units):
        return slice(first_unit * UNIT, (first_unit + units) * UNIT)

    def take_own(pairs):
        for u in pairs:
            xg[:, lanes_of(2 * u, 2)] = jnp.dot(hot1[:, :2 * BLK], cut(2 * u, 2, 0, 2), preferred_element_type=F32).astype(BF16)

    def take_a(e, units):
        mid = slice(e * HC, (e + 1) * HC)
        for u, n in units:
            cols = lanes_of(u, n)
            r = jnp.dot(hot1[mid, 2 * BLK:], cut(u, n, A, 1), preferred_element_type=F32)
            xg[mid, cols] = (xg[mid, cols].astype(F32) + r).astype(BF16)

    def first_tiles(h, e, first_unit, units, x, w_next=None):
        z = None
        for n in range(HID // TILE):
            cols = slice(n * TILE, (n + 1) * TILE)
            r = jnp.dot(x, win[e, first_unit * UNIT:(first_unit + units) * UNIT, cols], preferred_element_type=F32)
            if first_unit > 0:
                r = r + acc[e, :, cols]
            if first_unit + units < DIM // UNIT:
                acc[e, :, cols] = r
            else:
                part = gelu(r).astype(BF16)
                hid[h, e, :, cols] = part
                if w_next is not None:
                    step = jnp.dot(part, w_next[cols, :], preferred_element_type=F32)
                    z = step if z is None else z + step
        return z

    def first(e, first_unit, units, w_next=None):
        with scope(f"first{first_unit}e{e}"):
            for g in range(NG):
                if first_unit <= g * UG < first_unit + units:
                    wait_win(e, g)
            take_a(e, [(u, 2) for u in range(first_unit, first_unit + units, 2)])
            return first_tiles(0, e, first_unit, units, xg[e * HC:(e + 1) * HC, lanes_of(first_unit, units)], w_next)

    def first_late(g):
        for m in range(0, UG, 2):
            x = cut(UG * g + m, 2, 0, EP)
            xg2[:, m * UNIT:(m + 2) * UNIT] = jnp.dot(hot2[...], x, preferred_element_type=F32).astype(BF16)

        def body(e, _):
            first_tiles(1, e, UG * g, UG, xg2[pl.ds(pl.multiple_of(e * HC, HC), HC), :])
            return 0
        lax.fori_loop(0, OWN, body, 0)

    def second(m, r=None):
        h, j, e = order[m]
        n = h * NJ + j
        with scope(f"second{n}e{e}"):
            if m > 0:
                wait_wout(m)
            mid = slice(e * HC, (e + 1) * HC)
            if r is None:
                r = jnp.dot(hid[h, e], wout[m % NB], preferred_element_type=F32)
            snd[n, mid, :] = r[:, :NC]
            mine[n, mid, :] = r[:, NC:]
            copy_s(n, e).start()
            load_wout(m + NB)

    def ready(*ks):
        with scope(f"ready{ks[0]}"):
            @pl.when(follow)
            def _():
                for k in ks:
                    copy_c(k).wait_recv()
                    if k == NP - 1:
                        for g in range(NG):
                            copy_g(g).start()
                    if k < TWO_WAY:
                        copy_e(k).wait_recv()

    relay_b(2)
    with scope("pick0"):
        pick(0)
    relay_b(3)
    with scope("pick1"):
        pick(1)
    relay_b(4)
    with scope("wait_a"):
        near_x = xall.at[:, rows(place_near)]
        remote(near_x, near_x, 1, a_r.at[0], to_near).wait_recv()
    relay_d(0, 1)
    with scope("own0"):
        take_own(range(4))
    relay_b(5)
    with scope("own1"):
        take_own(range(4, 8))
    relay_d(2)
    relay_b(6)
    ready(0, 1, 2)
    first(0, 0, 4)
    for m in range(NB):
        load_wout(m)
    relay_b(7)
    relay_d(3, 4)
    ready(3, 4)
    first(0, 4, 4)
    relay_d(5)
    ready(5)
    first(0, 8, 2)
    relay_b(8)
    ready(8)
    first(0, 10, 2)
    relay_d(6)
    ready(6)
    first(0, 12, 2)
    wait_wout(0)
    relay_b(9)
    relay_d(7)
    ready(7, 9)
    second(0, first(0, 14, 2, wout.at[0]))
    for m in range(1, len(head)):
        second(m)
    first(1, 0, 4)
    first(1, 4, 4)
    first(1, 8, 4)
    first(1, 12, 4)
    copy_slots(to_near, core).start()
    copy_slots(to_far, there).start()
    copy_slots(to_diag, there).start()

    def relay_g(g):
        with scope(f"relayg{g}"):
            @pl.when(follow)
            def _():
                copy_g(g).wait_recv()
                copy_f(g).start()

    half = OWN * NJ
    for m in range(len(head), half):
        second(m)
        if m in (half - 8, half - 2):
            relay_g(0 if m == half - 8 else 1)
    with scope("pick_late"):
        pick_late()
    for g in range(NG):
        if g > 0 and g + 1 < NG:
            relay_g(g + 1)
        with scope(f"readyB{g}"):
            @pl.when(lead)
            def _():
                copy_f(g).wait_recv()
        with scope(f"firstB{g}"):
            first_late(g)
    def close(u):
        with scope(f"waits{u}"):
            wait_s(u)
        start, size = span(u)
        for n in range(start, start + size):
            zall[n, core] = (mine[n] + rcv[n]).astype(BF16)
        copy_zx(u, core, there).start()
        copy_zc(u, core).start()

    def forward(u):
        with scope(f"waitzx{u}"):
            copy_zx(u, place_far, place_far).wait_recv()
        copy_zf(u, place_far).start()

    def combine(j):
        total = jnp.zeros((BLK, NC), F32)
        for p in range(EP):
            for i in range(OWN):
                mid = slice(i * HC, (i + 1) * HC)
                z = jnp.concatenate([zall[j, p, mid, :], zall[NJ + j, p, mid, :]], axis=0)
                total = total + gate[p * OWN + i] * jnp.dot(back[p * OWN + i], z, preferred_element_type=F32)
        own = xall[tp * NJ + j, rows(core), :]
        res[j] = (own.astype(F32) + total).astype(BF16)
        if j > 0:
            copy_res(j, tp).start()
        else:
            @pl.when(lead)
            def _():
                copy_res(j, tp).start()

            @pl.when(follow)
            def _():
                copy_pass().start()
        out[:, pl.ds(pl.multiple_of(tp * HALF + j * NC, NC), NC)] = res[j]

    close(0)
    for m in range(half, 2 * half):
        second(m)


    with scope("slotwait"):
        three = slots.at[pl.ds(0, 3)]
        remote(three, three, 0, sl_r.at[0], to_near).wait_recv()
    with scope("back"):
        lanes = lax.broadcasted_iota(jnp.int32, (128, CAP), 1).astype(F32)
        for p in range(EP):
            mark = core if p < 2 else there
            owner = 2 * chip + p if p < 2 else 2 * (1 - chip) + (3 - p)
            for i in range(OWN):
                for c in range(BLK // 128):
                    part = slice(c * 128, (c + 1) * 128)
                    col = column(slots[p, pl.ds(i * 8 + mark * 2 + c, 1), :])
                    back[p * OWN + i, part, :] = jnp.where(jnp.concatenate([col, col], axis=1) == lanes, 1.0, 0.0).astype(BF16)
                    gate[p * OWN + i, part, :] = column(probs[pl.ds(owner * OWN + i, 1), :][:, part])

    units = len(SPANS)
    for u in range(1, units + 2):
        if u < units:
            close(u)
        if u - 2 >= EARLY_SPANS:
            with scope(f"waitzn{u - 2}"):
                if u - 2 == EARLY_SPANS:
                    wait_zn(0)
                wait_zn(u - 2)
            start, size = span(u - 2)
            for n in range(start, start + size):
                combine(n - NJ)
            if u - 2 == EARLY_SPANS + 1:
                @pl.when(lead)
                def _():
                    copy_pass().wait_recv()
                    copy_passed().start()
        if u - 1 < units:
            forward(u - 1)

    with scope("drain"):
        def left(ref, family):
            remote(ref, ref, family, res_r.at[0], to_near).wait_send()
        left(ltall.at[pl.ds(0, 3)], 4)
        left(slots.at[pl.ds(0, 3)], 0)
        left(zall.at[pl.ds(0, 12)], 1)
        left(zall.at[pl.ds(0, 12)], 2)
        left(zall.at[pl.ds(0, 10)], 3)

        @pl.when(lead)
        def _():
            left(passed, 5)
        remote(res, res, 3, res_r.at[0], to_peer).wait_recv()


def solution(mesh):
    def local_layer(tokens, logits, w_in, w_out):
        dma = pltpu.SemaphoreType.DMA
        units = len(SPANS)
        scratch = [
            pltpu.VMEM((DIM // UNIT, TOK, UNIT), BF16),
            pltpu.VMEM((EXPERTS, BLK), F32),
            pltpu.VMEM((EP, OWN, BLK), F32),
            pltpu.VMEM((EP, OWN, BLK), F32),
            pltpu.VMEM((EP, OWN * 8, 128), F32),
            pltpu.VMEM((OWN * HC, 3 * BLK), BF16),
            pltpu.VMEM((OWN * HC, TOK), BF16),
            pltpu.VMEM((OWN * HC, DIM), BF16),
            pltpu.VMEM((OWN * HC, KG), BF16),
            pltpu.VMEM((OWN, DIM, HID), BF16),
            pltpu.VMEM((OWN, HC, HID), F32),
            pltpu.VMEM((2, OWN, HC, HID), BF16),
            pltpu.VMEM((NB, HID, 2 * NC), BF16),
            pltpu.VMEM((2 * NJ, OWN * HC, NC), F32),
            pltpu.VMEM((2 * NJ, OWN * HC, NC), F32),
            pltpu.VMEM((2 * NJ, OWN * HC, NC), F32),
            pltpu.VMEM((2 * NJ, EP, OWN * HC, NC), BF16),
            pltpu.VMEM((EXPERTS, BLK, CAP), BF16),
            pltpu.VMEM((EXPERTS, BLK, NC), F32),
            pltpu.VMEM((EXPERTS, BLK), F32),
            pltpu.VMEM((NJ, BLK, NC), BF16),
            pltpu.VMEM((BLK, NC), BF16),
            dma((3,)), dma((3,)), dma((NB,)), dma((6,)),
            dma((1,)), dma((1,)), dma((1,)), dma((NP,)), dma((TWO_WAY,)), dma((NG,)),
            dma((units,)), dma((units,)), dma((1 + units - EARLY_SPANS,)), dma((1,)), dma((1,)),
        ]
        return pl.pallas_call(
            kernel,
            out_shape=pltpu.VMEM(tokens.shape, BF16),
            in_specs=[pl.BlockSpec(memory_space=pl.ANY), pl.BlockSpec(memory_space=pl.ANY),
                      pl.BlockSpec(memory_space=pl.ANY), pl.BlockSpec(memory_space=pl.ANY)],
            out_specs=pl.BlockSpec(memory_space=pltpu.VMEM),
            scratch_shapes=scratch,
            compiler_params=pltpu.CompilerParams(collective_id=0, has_side_effects=True,
                                                 vmem_limit_bytes=62_500_000),
            name="moe_layer",
        )(tokens, logits.T, w_in, w_out)

    row_spec = P(("dp", "ep"), None)
    return jax.shard_map(local_layer, mesh=mesh,
                         in_specs=(row_spec, row_spec, P("ep", None, "tp"), P("ep", "tp", None)),
                         out_specs=row_spec, check_vma=False)
```
